512 devices in a mesh: gx: 8 (over x, y_lo), gy: 8 (over y_hi, core), gz: 8 (over z).
Axes of the slice: x: 4, y: 8 (y_hi: 4, y_lo: 2; y = y_hi * 2 + y_lo), z: 8, core: 2. Of those that a mesh axis runs over, the one named last changes fastest.
Arguments:
- density: bfloat16 [8, 8, 8, 512, 256], P('gx', 'gy', 'gz'), may hold values from -6 to 6
- integrals: bfloat16 [8, 8, 8, 9, 512, 512], P('gx', 'gy', 'gz'), may hold values from -0.25 to 0.25
- offsets: int32 [8, 8, 8, 9], P('gx', 'gy', 'gz'), may hold values from 0 to 26, as said below
- counts: int32 [8, 8, 8], P('gx', 'gy', 'gz'), may hold values from 7 to 9, as said below
Outputs:
- exchange: bfloat16 [8, 8, 8, 512, 256], P('gx', 'gy', 'gz')
The draws below stay inside these ranges and needn't reach their ends.
Inputs may be any that keep to these rules, and one draw needn't show every extreme that they name: Slots from counts[p] on hold no tile of domain p; some domain has all 9 slots live in every draw. `offsets`: a code names one of the 27 domains within one step along each axis, as the steps say; the 9 codes of one domain are all different.
All inputs are finite; a program needn't handle non-finite values.
Results may differ from the reference program's by a relative error of at most 0.006.
Values may be sent and summed in bfloat16 or wider, within the bound.
A program may use at most 64 MiB of HBM per device.

```python
import jax
import jax.numpy as jnp
from jax import lax

BLK = 512
NCOL = 256
TCAP = 9
DX = 8
DY = 8
DZ = 8


def draw_counts(key, part):
    key_one = jax.random.fold_in(key, 11)
    key_three = jax.random.fold_in(key, 13)
    shape_all = (DX, DY, DZ)
    missing = jax.random.randint(key_one, shape_all, 0, (TCAP + 2) // 3)
    loads = TCAP - missing
    loads_flat = loads.reshape(-1)
    busiest = jax.random.randint(key_three, (), 0, DX * DY * DZ)
    loads_flat = loads_flat.at[busiest].set(TCAP)
    return loads_flat.reshape(shape_all).astype(jnp.int32)


def draw_offsets(key, part):
    key_perm = jax.random.fold_in(key, 21)
    domain_keys = jax.random.split(key_perm, DX * DY * DZ)
    rows = jax.vmap(lambda single: jax.random.permutation(single, 27)[:TCAP])(domain_keys)
    return rows.reshape(DX, DY, DZ, TCAP).astype(jnp.int32)


def levels(own_key, dims, cuts, smallest, top_value):
    level = 1.0
    for position, shards_of in cuts:
        draws = jax.random.uniform(jax.random.fold_in(jax.random.fold_in(own_key, 6), position), (shards_of,), jnp.float32, smallest / len(cuts), top_value / len(cuts))
        level = level * jnp.repeat(jnp.exp(draws), dims[position] // shards_of).reshape((-1,) + (1,) * (len(dims) - 1 - position))
    return level


def gaussian(rng, extent, deviation, limit, cuts=(), held_as=jnp.bfloat16):
    loudness = levels(rng, extent, cuts, -0.22, 0.18) if cuts else 1.0
    values = jax.random.normal(rng, extent, jnp.float32) * deviation * loudness
    return jnp.minimum(jnp.maximum(values, -limit), limit).astype(held_as)


def setup_inputs(seed: int = 0) -> dict:
    seeds = jax.random.split(jax.random.key(seed), 5)
    return {
        "density": gaussian(seeds[0], (DX, DY, DZ, BLK, NCOL), 1.0, 6.0, ((0, 8), (1, 8), (2, 8))),
        "integrals": gaussian(seeds[1], (DX, DY, DZ, TCAP, BLK, BLK), BLK ** -0.5, 0.25, ((0, 8), (1, 8), (2, 8))),
        "offsets": draw_offsets(jax.random.fold_in(seeds[4], 71), 0),
        "counts": draw_counts(jax.random.fold_in(seeds[4], 71), 0),
    }


def reference(density, integrals, offsets, counts):
    extent_x, extent_y, extent_z = density.shape[0], density.shape[1], density.shape[2]
    block_rows = density.shape[3]
    columns = density.shape[4]
    slot_total = integrals.shape[3]
    domains = extent_x * extent_y * extent_z
    dens_flat = density.reshape(domains, block_rows, columns)
    tile_flat = integrals.reshape(domains, slot_total, block_rows, block_rows)
    code_flat = offsets.reshape(domains, slot_total).astype(jnp.int32)
    live_flat = counts.reshape(domains).astype(jnp.int32)
    domain_ids = jnp.arange(domains, dtype=jnp.int32)
    coord_x = domain_ids // (extent_y * extent_z)
    coord_y = (domain_ids // extent_z) % extent_y
    coord_z = domain_ids % extent_z
    step_x = code_flat // 9 - 1
    step_y = (code_flat // 3) % 3 - 1
    step_z = code_flat % 3 - 1
    neighbour = (((coord_x[:, None] + step_x) % extent_x) * extent_y + (coord_y[:, None] + step_y) % extent_y) * extent_z + (coord_z[:, None] + step_z) % extent_z
    neighbour = neighbour.astype(jnp.int32)

    def visit_domain(total, item):
        tile_block, nbr_ids, live_count, home_index = item
        slot_live = (jnp.arange(slot_total, dtype=jnp.int32) < live_count).astype(jnp.float32)
        blocks = dens_flat[nbr_ids].astype(jnp.float32)
        tile_wide = tile_block.astype(jnp.float32) * slot_live[:, None, None]
        forward = jnp.einsum('sij,sjc->ic', tile_wide, blocks, precision=lax.Precision.HIGHEST)
        own_block = dens_flat[home_index].astype(jnp.float32)
        partial_value = jnp.einsum('sji,jc->sic', tile_wide, own_block, precision=lax.Precision.HIGHEST)
        partial_value = lax.optimization_barrier(partial_value.astype(jnp.bfloat16)).astype(jnp.float32)
        total = total.at[home_index].add(forward)
        total = total.at[nbr_ids].add(partial_value)
        return total, None

    start = jnp.zeros((domains, block_rows, columns), jnp.float32)
    total, _ = lax.scan(visit_domain, start, (tile_flat, neighbour, live_flat, domain_ids))
    return total.astype(jnp.bfloat16).reshape(density.shape)
```

```python
import functools

import jax
import jax.numpy as jnp
from jax import lax
from jax.experimental import pallas as pl
from jax.experimental.pallas import tpu as pltpu
from jax.sharding import PartitionSpec as P

MESH = pl.DeviceIdType.MESH
OWN, PAR, CRS = 0, 1, 2
CHUNKS = 2
ORDER = (
    0, 1, 30, 31, 32, 33, 34, 35, 36, 37, 38, 2, 3, 5, 39, 40, 41, 42, 43, 44, 45, 46, 47, 48, 53, 55, 68, 70,
    16, 17, 19, 52, 49, 10, 50, 51, 64, 65, 8, 66, 4, 6, 67, 13, 54, 22, 69, 18, 7, 20, 24, 9, 59, 27, 14, 56,
    11, 74, 58, 15, 71, 21, 28, 12, 61, 60, 57, 23, 29, 72, 25, 76, 26, 73, 62, 75, 79, 63, 77, 78,
)


def slot(group, dz, k):
    return ("H", group * 9 + dz * 3 + k)


def far(dz, k):
    return ("F", dz * 2 + k)


def out_slot(group, dz, k):
    return ("O", (group - 1) * 9 + dz * 3 + k)


class Task:
    def __init__(self, kind, q, waits=(), waits_s=(), waits_r=(), sends=(), cost=0.0, args=()):
        self.kind = kind
        self.q = q
        self.waits = list(waits)
        self.waits_s = list(waits_s)
        self.waits_r = list(waits_r)
        self.sends = list(sends)
        self.cost = cost
        self.args = args


def make_tasks(chunks):
    tasks = []
    for q in range(chunks):
        c = slot(0, 1, OWN)
        tasks.append(Task("relay", q, sends=[
            (c, slot(0, 1, PAR), "partner", None),
            (c, slot(0, 0, OWN), "zp", None),
            (c, slot(0, 2, OWN), "zm", None),
            (c, far(1, PAR), "outer", "S"),
            (c, slot(1, 1, OWN), "sib", None),
        ]))
    for q in range(chunks):
        c = slot(0, 1, PAR)
        tasks.append(Task("relay", q, [c], sends=[
            (c, slot(0, 1, CRS), "xd", None),
            (c, far(1, OWN), "outer", "S"),
            (c, slot(0, 0, PAR), "zp", None),
            (c, slot(0, 2, PAR), "zm", None),
            (c, slot(1, 1, PAR), "sib", None),
        ]))
        for dz in (0, 2):
            c = slot(0, dz, OWN)
            tasks.append(Task("relay", q, [c], sends=[
                (c, far(dz, PAR), "outer", "S"),
                (c, slot(1, dz, OWN), "sib", None),
            ]))
            c = slot(0, dz, PAR)
            tasks.append(Task("relay", q, [c], sends=[
                (c, far(dz, OWN), "outer", "S"),
                (c, slot(0, dz, CRS), "xd", None),
                (c, slot(1, dz, PAR), "sib", None),
            ]))
        for dz in (0, 1, 2):
            c = slot(0, dz, CRS)
            tasks.append(Task("relay", q, [c], sends=[(c, slot(1, dz, CRS), "sib", None)]))
        for k in (OWN, PAR):
            for dz in (1, 0, 2):
                c = far(dz, k)
                sends = []
                if dz == 1:
                    sends += [
                        (c, far(1, 1 - k), "partner", "R"),
                        (c, far(0, k), "zp", "S"),
                        (c, far(2, k), "zm", "S"),
                    ]
                if k == PAR:
                    sends.append((c, slot(2, dz, CRS), "sxd", None))
                sends.append((c, slot(2, dz, k), "sib", None))
                tasks.append(Task("relay", q, [c], sends=sends))
    tasks.append(Task("part", None, cost=3.5))
    for dz in (0, 2, 1):
        tasks.append(Task("sel", None, cost=0.12, args=(2, dz, CRS), sends=[
            (out_slot(2, dz, CRS), ("XF", dz), "sxp", None)]))
        for k in (PAR, OWN):
            tasks.append(Task("sel", None, cost=0.12, args=(2, dz, k), sends=[
                (out_slot(2, dz, k), ("RF", dz * 2 + k), "sib", None)]))
    for k in (CRS, PAR, OWN):
        for dz in (0, 2, 1):
            tasks.append(Task("sel", None, cost=0.12, args=(1, dz, k), sends=[
                (out_slot(1, dz, k), ("RN", dz * 3 + k), "sib", None)]))
    unit = 0.6 / chunks
    for q in range(chunks):
        for dz in (0, 2, 1):
            tasks.append(Task("cross", q, [("RN", dz * 3 + CRS)], cost=unit, args=(dz,), sends=[
                (("AX", dz), ("XN", dz), "xp", None)]))
        for dz in (0, 2):
            for k in (PAR, OWN):
                waits = [("RF", dz * 2 + k)]
                source = ("RF", dz * 2 + k)
                if k == PAR:
                    waits.append(("XF", dz))
                    source = ("AF", dz * 2 + k)
                tasks.append(Task("farz" if k == PAR else "relay", q, waits, cost=unit if k == PAR else 0.0,
                                  args=(dz,), sends=[
                    (source, ("ZF", (0 if dz == 0 else 2) + k), "zm" if dz == 0 else "zp", "S"),
                    (source, ("EN", dz * 2 + 1 - k), "outer", "R")]))
        for k in (PAR, OWN):
            waits = [("RF", 2 + k)] + ([("XF", 1)] if k == PAR else [])
            tasks.append(Task("farc", q, waits, [("ZF", k), ("ZF", 2 + k)], [("IF", k)], cost=unit * 1.3,
                              args=(k,), sends=[
                (("AF", 2 + k), ("IF", 1 - k), "partner", "S"),
                (("AF", 2 + k), ("EN", 3 - k), "outer", "R")]))
        for dz in (0, 2):
            for k in (PAR, OWN):
                waits = [("RN", dz * 3 + k)] + ([("XN", dz)] if k == PAR else [])
                tasks.append(Task("nearz", q, waits, [("EN", dz * 2 + k)], cost=unit * 1.3, args=(dz, k), sends=[
                    (("AZ", dz + k), ("ZN", (0 if dz == 0 else 2) + k), "zm" if dz == 0 else "zp", None)]))
        tasks.append(Task("nearp", q, [("RN", 3 + PAR), ("XN", 1), ("ZN", PAR), ("ZN", 2 + PAR)],
                          [("EN", 2 + PAR)], cost=unit * 1.6, sends=[
            (("AI", 0), ("IN", 0), "partner", None)]))
        tasks.append(Task("last", q, [("RN", 3 + OWN), ("ZN", OWN), ("ZN", 2 + OWN), ("IN", 0)],
                          [("EN", 2 + OWN)], cost=unit * 1.6))
    tasks.append(Task("forward", None, [("H", i) for i in range(27) if i != 3], cost=3.0))
    return tasks


BUFFERS = {
    "H": (28, True), "F": (6, True),
    "O": (18, False), "AX": (3, False), "AF": (6, False), "AZ": (4, False), "AI": (1, False),
    "RN": (9, False), "RF": (6, False), "XN": (3, False), "XF": (3, False), "ZF": (4, False),
    "IF": (2, False), "EN": (6, False), "ZN": (4, False), "IN": (1, False),
}
RECEIVED = ("H", "F", "RN", "RF", "XN", "XF", "ZF", "IF", "EN", "ZN", "IN")


def kernel(chunks, order, off_ref, cnt_ref, dens_ref, tile_hbm, out_ref, *scratch):
    names = list(BUFFERS)
    buf = dict(zip(names, scratch[:len(names)]))
    tiles, part, flip, total, back, chosen, local_sem, send_sem, recv_sem = scratch[len(names):]
    gx, gy, gz = lax.axis_index("gx"), lax.axis_index("gy"), lax.axis_index("gz")
    nx, ny, nz = lax.axis_size("gx"), lax.axis_size("gy"), lax.axis_size("gz")
    b, c = lax.rem(gx, 2), lax.rem(gy, 2)
    sender = b == c
    receiver = b != c
    xd = lax.rem(gx + 2 - 4 * b + nx, nx)
    xp = lax.rem(gx - 2 + 4 * b + nx, nx)
    sib = gy + 1 - 2 * c
    outer_x = lax.rem(gx + 1 - 2 * b + nx, nx)
    where_to = {
        "partner": (outer_x, gy, gz),
        "outer": (outer_x, lax.rem(gy - 2 + 4 * b + ny, ny), gz),
        "sib": (gx, sib, gz),
        "xd": (xd, gy, gz), "xp": (xp, gy, gz),
        "sxd": (xd, sib, gz), "sxp": (xp, sib, gz),
        "zp": (gx, gy, lax.rem(gz + 1, nz)),
        "zm": (gx, gy, lax.rem(gz + nz - 1, nz)),
    }
    rows, columns = buf["H"].shape[1:]
    slots = tiles.shape[0]

    density_copy = pltpu.make_async_copy(dens_ref.at[0, 0, 0], buf["H"].at[3], local_sem.at[slots])
    density_copy.start()
    for s in range(slots):
        pltpu.make_async_copy(tile_hbm.at[0, 0, 0, s], tiles.at[s], local_sem.at[s]).start()
    barrier = pltpu.get_barrier_semaphore()
    for target in where_to.values():
        pl.semaphore_signal(barrier, inc=1, device_id=target, device_id_type=MESH)

    live = cnt_ref[0, 0, 0]
    home = []
    for s in range(slots):
        code = off_ref[0, 0, 0, s]
        dx, dy, dz = lax.div(code, 9), lax.rem(lax.div(code, 3), 3), lax.rem(code, 3)
        k = jnp.where(dx == 1, OWN, jnp.where(dx == 2 - 2 * b, PAR, CRS))
        group = jnp.where(dy == 1, 0, jnp.where(dy == 2 - 2 * c, 1, 2))
        home.append(jnp.where(s < live, group * 9 + dz * 3 + k, 27))
        chosen[27 + s] = home[s]

    @pl.loop(0, 27)
    def _(h):
        index = jnp.int32(slots)
        for s in range(slots):
            index = jnp.where(home[s] == h, s, index)
        chosen[h] = index

    buf["H"][27] = jnp.zeros((rows, columns), jnp.bfloat16)
    part[slots] = jnp.zeros((columns, rows), jnp.bfloat16)
    density_copy.wait()
    pl.semaphore_wait(barrier, len(where_to))

    def piece(name, index, q):
        size = (rows if BUFFERS[name][1] else columns) // chunks
        return buf[name].at[index, pl.ds(q * size, size)]

    first_sem = {}
    count = 0
    for name in RECEIVED:
        first_sem[name] = count
        count += BUFFERS[name][0] * chunks

    def arrival(name, index, q):
        return recv_sem.at[first_sem[name] + index * chunks + q]

    waited = set()

    def wait_for(key, q):
        if (key, q) in waited:
            return
        waited.add((key, q))
        ref = piece(key[0], key[1], q)
        pltpu.make_async_copy(ref, ref, arrival(key[0], key[1], q)).wait()

    in_flight = []

    def send(item, q):
        source, target, to, role = item
        copy = pltpu.make_async_remote_copy(
            src_ref=piece(source[0], source[1], q),
            dst_ref=piece(target[0], target[1], q),
            send_sem=send_sem.at[len(in_flight)],
            recv_sem=arrival(target[0], target[1], q),
            device_id=where_to[to],
            device_id_type=MESH,
        )
        in_flight.append((copy, role))
        return copy

    strip = 32
    height = columns // chunks

    def add(target, q, terms, own=None):
        @pl.loop(0, height // strip)
        def _(i):
            span = pl.ds(pl.multiple_of(q * height + i * strip, strip), strip)
            value = None
            if own is not None:
                value = part[chosen[own], span].astype(jnp.float32)
            for name, index in terms:
                term = buf[name][index, span].astype(jnp.float32)
                value = term if value is None else value + term
            if target is None:
                back[span] = value
            else:
                buf[target[0]][target[1], span] = value.astype(jnp.bfloat16)

    def partials():
        flip[...] = buf["H"][3].T

        @pl.loop(0, slots)
        def _(s):
            pltpu.make_async_copy(tile_hbm.at[0, 0, 0, s], tiles.at[s], local_sem.at[s]).wait()
            part[s] = jnp.dot(flip[...], tiles[s], preferred_element_type=jnp.float32).astype(jnp.bfloat16)

    def forward():
        total[...] = jnp.zeros_like(total)

        @pl.loop(0, slots)
        def _(s):
            total[...] += jnp.dot(tiles[s], buf["H"][chosen[27 + s]], preferred_element_type=jnp.float32)

    tasks = make_tasks(chunks)
    for number in order:
        task = tasks[number]
        spans = range(chunks) if task.q is None else [task.q]
        for key in task.waits:
            for q in spans:
                wait_for(key, q)
        q = task.q
        kind, args = task.kind, task.args
        by_role = {}
        if kind == "part":
            partials()
        elif kind == "forward":
            forward()
        elif kind == "sel":
            group, dz, k = args
            buf["O"][(group - 1) * 9 + dz * 3 + k] = part[chosen[group * 9 + dz * 3 + k]]
        elif kind == "cross":
            add(("AX", args[0]), q, [("RN", args[0] * 3 + CRS)], own=args[0] * 3 + CRS)
        elif kind == "farz":
            dz = args[0]
            add(("AF", dz * 2 + PAR), q, [("RF", dz * 2 + PAR), ("XF", dz)])
        elif kind == "farc":
            k = args[0]
            terms = [("RF", 2 + k)] + ([("XF", 1)] if k == PAR else [])
            by_role["S"] = functools.partial(add, ("AF", 2 + k), q, terms + [("ZF", k), ("ZF", 2 + k)])
            by_role["R"] = functools.partial(add, ("AF", 2 + k), q, terms + [("IF", k)])
        elif kind == "nearz":
            dz, k = args
            terms = [("RN", dz * 3 + k)] + ([("XN", dz)] if k == PAR else [])
            by_role["S"] = functools.partial(add, ("AZ", dz + k), q, terms + [("EN", dz * 2 + k)], own=dz * 3 + k)
            by_role["R"] = functools.partial(add, ("AZ", dz + k), q, terms, own=dz * 3 + k)
        elif kind == "nearp":
            terms = [("RN", 3 + PAR), ("XN", 1), ("ZN", PAR), ("ZN", 2 + PAR)]
            by_role["S"] = functools.partial(add, ("AI", 0), q, terms + [("EN", 2 + PAR)], own=3 + PAR)
            by_role["R"] = functools.partial(add, ("AI", 0), q, terms, own=3 + PAR)
        elif kind == "last":
            terms = [("RN", 3 + OWN), ("ZN", OWN), ("ZN", 2 + OWN), ("IN", 0)]
            by_role["S"] = functools.partial(add, None, q, terms + [("EN", 2 + OWN)], own=3 + OWN)
            by_role["R"] = functools.partial(add, None, q, terms, own=3 + OWN)

        copies = {None: [], "S": [], "R": []}
        for item in task.sends:
            for span in spans:
                copies[item[3]].append(send(item, span))
        for role, flag, keys in (("S", sender, task.waits_s), ("R", receiver, task.waits_r)):
            if keys or copies[role] or role in by_role:
                @pl.when(flag)
                def _():
                    for key in keys:
                        for span in spans:
                            wait_for(key, span)
                    if role in by_role:
                        by_role[role]()
                    for copy in copies[role]:
                        copy.start()
        for copy in copies[None]:
            copy.start()

    out_ref[0, 0, 0] = (total[...] + back[...].T).astype(out_ref.dtype)
    for role, flag in ((None, None), ("S", sender), ("R", receiver)):
        def drain():
            for copy, which in in_flight:
                if which == role:
                    copy.wait_send()
        if role is None:
            drain()
        else:
            pl.when(flag)(drain)


def local(density, integrals, offsets, counts):
    rows, columns = density.shape[3:]
    slots = integrals.shape[3]
    tasks = make_tasks(CHUNKS)
    sends = sum(len(t.sends) * (CHUNKS if t.q is None else 1) for t in tasks)
    arrivals = sum(BUFFERS[name][0] for name in RECEIVED) * CHUNKS
    scratch = [
        pltpu.VMEM((n, rows, columns) if straight else (n, columns, rows), jnp.bfloat16)
        for n, straight in BUFFERS.values()
    ]
    scratch += [
        pltpu.VMEM((slots, rows, rows), jnp.bfloat16),
        pltpu.VMEM((slots + 1, columns, rows), jnp.bfloat16),
        pltpu.VMEM((columns, rows), jnp.bfloat16),
        pltpu.VMEM((rows, columns), jnp.float32),
        pltpu.VMEM((columns, rows), jnp.float32),
        pltpu.SMEM((27 + slots,), jnp.int32),
        pltpu.SemaphoreType.DMA((slots + 1,)),
        pltpu.SemaphoreType.DMA((sends,)),
        pltpu.SemaphoreType.DMA((arrivals,)),
    ]
    return pl.pallas_call(
        functools.partial(kernel, CHUNKS, ORDER),
        out_shape=jax.ShapeDtypeStruct(density.shape, density.dtype),
        in_specs=[
            pl.BlockSpec(memory_space=pltpu.SMEM),
            pl.BlockSpec(memory_space=pltpu.SMEM),
            pl.BlockSpec(memory_space=pl.ANY),
            pl.BlockSpec(memory_space=pl.ANY),
        ],
        out_specs=pl.BlockSpec(memory_space=pltpu.VMEM),
        scratch_shapes=scratch,
        compiler_params=pltpu.CompilerParams(
            collective_id=0, has_side_effects=True, vmem_limit_bytes=56 * 1024 * 1024
        ),
    )(offsets, counts, density, integrals)


def solution(mesh):
    return jax.shard_map(
        local,
        mesh=mesh,
        in_specs=(
            P("gx", "gy", "gz", None, None),
            P("gx", "gy", "gz", None, None, None),
            P("gx", "gy", "gz", None),
            P("gx", "gy", "gz"),
        ),
        out_specs=P("gx", "gy", "gz", None, None),
        check_vma=False,
    )
```

```python
import functools

import jax
import jax.numpy as jnp
from jax import lax
from jax.experimental import pallas as pl
from jax.experimental.pallas import tpu as pltpu
from jax.sharding import PartitionSpec as P

MESH = pl.DeviceIdType.MESH
OWN, PAR, CRS = 0, 1, 2
VMEM_LIMIT = 56164352
D_SIZES = (4, 4, 8)
P_SIZES = (8, 8)
X_FIRST = ()
ORDER = {
    "S": (
        0, 1, 2, 45, 46, 47, 48, 49, 50, 51, 52, 53, 3, 4, 6, 54, 55, 56, 57, 58, 59, 60, 61, 62, 63, 69,
        17, 18, 20, 90, 73, 94, 8, 77, 98, 64, 85, 31, 32, 34, 65, 67, 86, 22, 5, 7, 11, 19, 21, 25, 88, 36,
        33, 39, 71, 9, 14, 10, 80, 28, 66, 92, 23, 24, 101, 42, 35, 87, 75, 12, 13, 37, 82, 26, 27, 96, 106,
        103, 40, 41, 15, 16, 107, 29, 38, 79, 43, 30, 100, 84, 81, 105, 44, 102, 83, 104, 108,
    ),
    "R": (
        0, 1, 2, 45, 14, 46, 47, 48, 49, 50, 51, 52, 3, 4, 6, 28, 53, 54, 55, 56, 57, 58, 59, 60, 61, 62,
        63, 17, 18, 20, 42, 11, 15, 64, 8, 85, 16, 31, 32, 34, 65, 86, 79, 100, 25, 29, 81, 5, 7, 102, 22,
        30, 80, 101, 82, 68, 19, 21, 103, 39, 43, 89, 33, 44, 72, 66, 12, 36, 13, 93, 35, 87, 26, 9, 76, 27,
        10, 97, 70, 40, 23, 91, 83, 24, 74, 41, 104, 95, 78, 37, 106, 99, 38, 107, 108, 84, 105,
    ),
}


def slot(group, dz, k):
    return ("H", group * 9 + dz * 3 + k)


def far(dz, k):
    return ("F", dz * 2 + k)


def out_slot(group, dz, k):
    return ("O", (group - 1) * 9 + dz * 3 + k)


class Task:
    def __init__(self, kind, q, waits=(), waits_s=(), waits_r=(), sends=(), cost=0.0, args=(), role=None):
        self.kind = kind
        self.q = q
        self.waits = list(waits)
        self.waits_s = list(waits_s)
        self.waits_r = list(waits_r)
        self.sends = list(sends)
        self.cost = cost
        self.args = args
        self.role = role


def make_tasks(d_sizes, p_sizes, x_first=()):
    tasks = []
    for q in range(len(d_sizes)):
        c = slot(0, 1, OWN)
        tasks.append(Task("relay", q, sends=[
            (c, slot(0, 1, PAR), "partner", None),
            (c, slot(0, 0, OWN), "zp", None),
            (c, slot(0, 2, OWN), "zm", None),
            (c, far(1, PAR), "outer", "S"),
            (c, slot(1, 1, OWN), "sib", None),
        ]))
    for q in range(len(d_sizes)):
        c = slot(0, 1, PAR)
        tasks.append(Task("relay", q, [c], sends=[
            (c, slot(0, 1, CRS), "xd", None),
            (c, far(1, OWN), "outer", "S"),
            (c, slot(0, 0, PAR), "zp", None),
            (c, slot(0, 2, PAR), "zm", None),
            (c, slot(1, 1, PAR), "sib", None),
        ]))
        for dz in (0, 2):
            c = slot(0, dz, OWN)
            tasks.append(Task("relay", q, [c], sends=[
                (c, far(dz, PAR), "outer", "S"),
                (c, slot(1, dz, OWN), "sib", None),
            ]))
            c = slot(0, dz, PAR)
            sends = [(c, far(dz, OWN), "outer", "S")]
            if q not in x_first:
                sends.append((c, slot(0, dz, CRS), "xd", None))
            sends.append((c, slot(1, dz, PAR), "sib", None))
            tasks.append(Task("relay", q, [c], sends=sends))
        for dz in (1, 0, 2):
            c = slot(0, dz, CRS)
            sends = [(c, slot(1, dz, CRS), "sib", None)]
            if dz == 1 and q in x_first:
                sends = [(c, slot(0, 0, CRS), "zp", None), (c, slot(0, 2, CRS), "zm", None)] + sends
            tasks.append(Task("relay", q, [c], sends=sends))
        for k in (OWN, PAR):
            for dz in (1, 0, 2):
                c = far(dz, k)
                sends = []
                if dz == 1:
                    sends += [
                        (c, far(1, 1 - k), "partner", "R"),
                        (c, far(0, k), "zp", "S"),
                        (c, far(2, k), "zm", "S"),
                    ]
                if k == PAR:
                    sends.append((c, slot(2, dz, CRS), "sxd", None))
                sends.append((c, slot(2, dz, k), "sib", None))
                tasks.append(Task("relay", q, [c], sends=sends))
    tasks.append(Task("part", None, cost=2.9))
    for dz in (0, 2, 1):
        for k in (CRS, PAR, OWN):
            send = (out_slot(2, dz, k), ("RF", dz * 2 + k), "sib", None)
            if k == CRS:
                send = (out_slot(2, dz, k), ("XF", dz), "sxp", None)
            tasks.append(Task("sel", None, cost=0.03, args=(2, dz, k), sends=[send]))
    for k in (CRS, PAR, OWN):
        for dz in (0, 2, 1):
            tasks.append(Task("sel", None, cost=0.03, args=(1, dz, k), sends=[
                (out_slot(1, dz, k), ("RN", dz * 3 + k), "sib", None)]))
    for q, size in enumerate(p_sizes):
        unit = 0.14 * size / 16
        for dz in (0, 2):
            tasks.append(Task("add", q, [("RN", dz * 3 + CRS)], cost=unit, args=(("AX", dz), dz * 3 + CRS), sends=[
                (("AX", dz), ("ZX", dz // 2), "zm" if dz == 0 else "zp", None)]))
        tasks.append(Task("add", q, [("RN", 3 + CRS), ("ZX", 0), ("ZX", 1)], cost=unit * 1.5,
                          args=(("AX", 1), 3 + CRS), sends=[(("AX", 1), ("XN", 0), "xp", None)]))
        for dz in (0, 2, 1):
            for k in (PAR, OWN):
                here = ("AF", dz * 2 + k)
                waits = [("RF", dz * 2 + k)] + ([("XF", dz)] if k == PAR else [])
                if k == PAR:
                    tasks.append(Task("add", q, waits_s=waits, role="S", cost=unit, args=(here, None), sends=[
                        (here, ("IF", dz * 2 + 1 - k), "partner", "S")]))
                else:
                    tasks.append(Task("relay", q, waits_s=waits, role="S", sends=[
                        (waits[0], ("IF", dz * 2 + 1 - k), "partner", "S")]))
                tasks.append(Task("add", q, waits_r=waits + [("IF", dz * 2 + k)], role="R", cost=unit * 1.2,
                                  args=(here, None), sends=[(here, ("EN", dz * 2 + 1 - k), "outer", "R")]))
        for dz in (0, 2):
            for k in (PAR, OWN):
                tasks.append(Task("add", q, [("RN", dz * 3 + k)], [("EN", dz * 2 + k)], cost=unit * 1.2,
                                  args=(("AZ", dz + k), dz * 3 + k), sends=[
                    (("AZ", dz + k), ("ZN", dz + k), "zm" if dz == 0 else "zp", None)]))
        tasks.append(Task("add", q, [("RN", 3 + PAR), ("XN", 0), ("ZN", PAR), ("ZN", 2 + PAR)],
                          [("EN", 2 + PAR)], cost=unit * 1.6, args=(("AI", 0), 3 + PAR), sends=[
            (("AI", 0), ("IN", 0), "partner", None)]))
        tasks.append(Task("add", q, [("RN", 3 + OWN), ("ZN", OWN), ("ZN", 2 + OWN), ("IN", 0)],
                          [("EN", 2 + OWN)], cost=unit * 1.6, args=(None, 3 + OWN)))
    for q, size in enumerate(d_sizes):
        tasks.append(Task("forward", q, [("H", i) for i in range(27) if i != 3], cost=0.2 + 2.7 * size / 16))
    return tasks


BUFFERS = {
    "H": (28, True), "F": (6, True),
    "O": (18, False), "AX": (3, False), "AF": (6, False), "AZ": (4, False), "AI": (1, False),
    "RN": (9, False), "RF": (6, False), "XN": (1, False), "XF": (3, False), "ZX": (2, False),
    "IF": (6, False), "EN": (6, False), "ZN": (4, False), "IN": (1, False),
}
RECEIVED = ("H", "F", "RN", "RF", "XN", "XF", "ZX", "IF", "EN", "ZN", "IN")


def chunks_of(name):
    sizes = D_SIZES if BUFFERS[name][1] else P_SIZES
    return [(sum(sizes[:i]), size) for i, size in enumerate(sizes)]


def places(name, rows, columns):
    unit = (rows if BUFFERS[name][1] else columns) // 16
    return [(first * unit, size * unit) for first, size in chunks_of(name)]


def kernel(off_hbm, cnt_hbm, dens_ref, tile_hbm, out_ref, *scratch):
    names = list(BUFFERS)
    halo = scratch[:len(D_SIZES)]
    scratch = scratch[len(D_SIZES):]
    buf = dict(zip(names[1:], scratch[:len(names) - 1]))
    tiles = scratch[len(names) - 1:len(names) - 1 + len(D_SIZES)]
    (square, part, flip, picked, total, back, off_ref, cnt_ref, chosen,
     local_sem, tile_sem, send_sem, recv_sem) = scratch[len(names) - 1 + len(D_SIZES):]
    gx, gy, gz = lax.axis_index("gx"), lax.axis_index("gy"), lax.axis_index("gz")
    nx, ny, nz = lax.axis_size("gx"), lax.axis_size("gy"), lax.axis_size("gz")
    b, c = lax.rem(gx, 2), lax.rem(gy, 2)
    xd = lax.rem(gx + 2 - 4 * b + nx, nx)
    xp = lax.rem(gx - 2 + 4 * b + nx, nx)
    sib = gy + 1 - 2 * c
    outer_x = lax.rem(gx + 1 - 2 * b + nx, nx)
    where_to = {
        "partner": (outer_x, gy, gz),
        "outer": (outer_x, lax.rem(gy - 2 + 4 * b + ny, ny), gz),
        "sib": (gx, sib, gz),
        "xd": (xd, gy, gz), "xp": (xp, gy, gz),
        "sxd": (xd, sib, gz), "sxp": (xp, sib, gz),
        "zp": (gx, gy, lax.rem(gz + 1, nz)),
        "zm": (gx, gy, lax.rem(gz + nz - 1, nz)),
    }
    rows, columns = total.shape
    slots = off_ref.shape[-1]
    d_places = places("H", rows, columns)

    barrier = pltpu.get_barrier_semaphore()
    for target in where_to.values():
        pl.semaphore_signal(barrier, inc=1, device_id=target, device_id_type=MESH)
    density_copies = []
    for q, (first, size) in enumerate(d_places):
        copy = pltpu.make_async_copy(
            dens_ref.at[0, 0, 0, pl.ds(first, size)], halo[q].at[3], local_sem.at[slots + q])
        copy.start()
        density_copies.append(copy)
    index_copies = [
        pltpu.make_async_copy(off_hbm, off_ref, local_sem.at[slots + len(d_places)]),
        pltpu.make_async_copy(cnt_hbm, cnt_ref, local_sem.at[slots + len(d_places) + 1]),
    ]
    for copy in index_copies:
        copy.start()

    def tile_copy(s, q):
        first, size = d_places[q]
        return pltpu.make_async_copy(
            tile_hbm.at[0, 0, 0, s, :, pl.ds(first, size)], tiles[q].at[:, pl.ds(s * size, size)],
            tile_sem.at[s * len(d_places) + q])

    for s in range(slots):
        pltpu.make_async_copy(tile_hbm.at[0, 0, 0, s], square.at[s], local_sem.at[s]).start()

    def piece(name, index, q):
        if name == "H":
            return halo[q].at[index]
        first, size = places(name, rows, columns)[q]
        return buf[name].at[index, pl.ds(first, size)]

    first_sem = {}
    count = 0
    for name in RECEIVED:
        first_sem[name] = count
        count += BUFFERS[name][0] * len(chunks_of(name))

    def arrival(name, index, q):
        return recv_sem.at[first_sem[name] + index * len(chunks_of(name)) + q]

    def add(target, q, terms, own):
        first, size = places("AF", rows, columns)[q]
        strip = 32

        @pl.loop(0, size // strip)
        def _(i):
            span = pl.ds(pl.multiple_of(first + i * strip, strip), strip)
            value = None
            if own is not None:
                value = part[chosen[own], span].astype(jnp.float32)
            for name, index in terms:
                term = buf[name][index, span].astype(jnp.float32)
                value = term if value is None else value + term
            if target is None:
                back[span] = value
            else:
                buf[target[0]][target[1], span] = value.astype(jnp.bfloat16)

    def find_tiles():
        live = cnt_ref[0, 0, 0]
        home = []
        for s in range(slots):
            code = off_ref[0, 0, 0, s]
            dx, dy, dz = lax.div(code, 9), lax.rem(lax.div(code, 3), 3), lax.rem(code, 3)
            k = jnp.where(dx == 1, OWN, jnp.where(dx == 2 - 2 * b, PAR, CRS))
            group = jnp.where(dy == 1, 0, jnp.where(dy == 2 - 2 * c, 1, 2))
            home.append(jnp.where(s < live, group * 9 + dz * 3 + k, 27))
            chosen[27 + s] = home[s]

        @pl.loop(0, 27)
        def _(h):
            index = jnp.int32(slots)
            for s in range(slots):
                index = jnp.where(home[s] == h, s, index)
            chosen[h] = index

    def partials():
        for q, (first, size) in enumerate(d_places):
            flip[:, first:first + size] = halo[q][3].T
            halo[q][27] = jnp.zeros((size, columns), jnp.bfloat16)
        part[slots] = jnp.zeros((columns, rows), jnp.bfloat16)
        total[...] = jnp.zeros_like(total)
        for copy in index_copies:
            copy.wait()
        find_tiles()

        @pl.loop(0, slots)
        def _(s):
            pltpu.make_async_copy(tile_hbm.at[0, 0, 0, s], square.at[s], local_sem.at[s]).wait()
            part[s] = jnp.dot(flip[...], square[s], preferred_element_type=jnp.float32).astype(jnp.bfloat16)

        for s in range(slots):
            for q in range(len(d_places)):
                tile_copy(s, q).start()

    def forward(q):
        size = d_places[q][1]
        for s in range(slots):
            tile_copy(s, q).wait()
            picked[s * size:(s + 1) * size] = halo[q][chosen[27 + s]]
        total[...] += jnp.dot(tiles[q][...], picked[:slots * size], preferred_element_type=jnp.float32)

    tasks = make_tasks(D_SIZES, P_SIZES, X_FIRST)

    def run(role):
        waited = set()
        in_flight = []
        for number in ORDER[role]:
            task = tasks[number]
            keys = task.waits + (task.waits_s if role == "S" else task.waits_r)
            for name, index in keys:
                if (name, index, task.q) not in waited:
                    waited.add((name, index, task.q))
                    ref = piece(name, index, task.q)
                    pltpu.make_async_copy(ref, ref, arrival(name, index, task.q)).wait()
            if task.kind == "part":
                partials()
            elif task.kind == "forward":
                forward(task.q)
            elif task.kind == "sel":
                group, dz, k = task.args
                buf["O"][(group - 1) * 9 + dz * 3 + k] = part[chosen[group * 9 + dz * 3 + k]]
            elif task.kind == "add":
                add(task.args[0], task.q, keys, task.args[1])
            elif number < len(D_SIZES):
                density_copies[number].wait()
            for source, target, to, only in task.sends:
                if only in (None, role):
                    for q in range(len(P_SIZES)) if task.q is None else [task.q]:
                        copy = pltpu.make_async_remote_copy(
                            src_ref=piece(source[0], source[1], q),
                            dst_ref=piece(target[0], target[1], q),
                            send_sem=send_sem.at[len(in_flight)],
                            recv_sem=arrival(target[0], target[1], q),
                            device_id=where_to[to],
                            device_id_type=MESH,
                        )
                        copy.start()
                        in_flight.append(copy)
        out_ref[0, 0, 0] = (total[...] + back[...].T).astype(out_ref.dtype)
        for copy in in_flight:
            copy.wait_send()

    pl.semaphore_wait(barrier, len(where_to))
    pl.when(b == c)(functools.partial(run, "S"))
    pl.when(b != c)(functools.partial(run, "R"))


def local(density, integrals, offsets, counts):
    rows, columns = density.shape[3:]
    slots = integrals.shape[3]
    tasks = make_tasks(D_SIZES, P_SIZES, X_FIRST)
    sends = sum(len(t.sends) * (len(P_SIZES) if t.q is None else 1) for t in tasks)
    arrivals = sum(BUFFERS[name][0] * len(chunks_of(name)) for name in RECEIVED)
    scratch = [pltpu.VMEM((BUFFERS["H"][0], size, columns), jnp.bfloat16) for _, size in places("H", rows, columns)]
    scratch += [
        pltpu.VMEM((n, rows, columns) if straight else (n, columns, rows), jnp.bfloat16)
        for name, (n, straight) in BUFFERS.items() if name != "H"
    ]
    scratch += [
        pltpu.VMEM((rows, slots * size), jnp.bfloat16) for _, size in places("H", rows, columns)
    ]
    scratch += [
        pltpu.VMEM((slots, rows, rows), jnp.bfloat16),
        pltpu.VMEM((slots + 1, columns, rows), jnp.bfloat16),
        pltpu.VMEM((columns, rows), jnp.bfloat16),
        pltpu.VMEM((slots * max(size for _, size in places("H", rows, columns)), columns), jnp.bfloat16),
        pltpu.VMEM((rows, columns), jnp.float32),
        pltpu.VMEM((columns, rows), jnp.float32),
        pltpu.SMEM(offsets.shape, jnp.int32),
        pltpu.SMEM(counts.shape, jnp.int32),
        pltpu.SMEM((27 + slots,), jnp.int32),
        pltpu.SemaphoreType.DMA((slots + len(D_SIZES) + 2,)),
        pltpu.SemaphoreType.DMA((slots * len(D_SIZES),)),
        pltpu.SemaphoreType.DMA((sends,)),
        pltpu.SemaphoreType.DMA((arrivals,)),
    ]
    return pl.pallas_call(
        kernel,
        out_shape=jax.ShapeDtypeStruct(density.shape, density.dtype),
        in_specs=[
            pl.BlockSpec(memory_space=pl.ANY),
            pl.BlockSpec(memory_space=pl.ANY),
            pl.BlockSpec(memory_space=pl.ANY),
            pl.BlockSpec(memory_space=pl.ANY),
        ],
        out_specs=pl.BlockSpec(memory_space=pltpu.VMEM),
        scratch_shapes=scratch,
        compiler_params=pltpu.CompilerParams(
            collective_id=0, has_side_effects=True, vmem_limit_bytes=VMEM_LIMIT
        ),
    )(offsets, counts, density, integrals)


def solution(mesh):
    return jax.shard_map(
        local,
        mesh=mesh,
        in_specs=(
            P("gx", "gy", "gz", None, None),
            P("gx", "gy", "gz", None, None, None),
            P("gx", "gy", "gz", None),
            P("gx", "gy", "gz"),
        ),
        out_specs=P("gx", "gy", "gz", None, None),
        check_vma=False,
    )
```

```python
import functools

import jax
import jax.numpy as jnp
from jax import lax
from jax.experimental import pallas as pl
from jax.experimental.pallas import tpu as pltpu
from jax.sharding import PartitionSpec as P

MESH = pl.DeviceIdType.MESH
OWN, PAR, CRS = 0, 1, 2
VMEM_LIMIT = 56164352
D_SIZES = (4, 4, 8)
P_SIZES = (8, 8)
X_FIRST = ()
ORDER = {
    "S": (
        0, 1, 2, 45, 46, 47, 48, 49, 50, 51, 52, 53, 3, 4, 6, 54, 55, 56, 57, 58, 59, 60, 61, 62, 63, 69,
        17, 18, 20, 90, 73, 94, 8, 77, 98, 64, 85, 31, 32, 34, 65, 67, 86, 22, 5, 7, 11, 19, 21, 25, 88, 36,
        33, 39, 71, 9, 14, 10, 80, 28, 66, 92, 23, 24, 101, 42, 35, 87, 75, 12, 13, 37, 82, 26, 27, 96, 106,
        103, 40, 41, 15, 16, 107, 29, 38, 79, 43, 30, 100, 84, 81, 105, 44, 102, 83, 104, 108,
    ),
    "R": (
        0, 1, 2, 45, 14, 46, 47, 48, 49, 50, 51, 52, 3, 4, 6, 28, 53, 54, 55, 56, 57, 58, 59, 60, 61, 62,
        63, 17, 18, 20, 42, 11, 15, 64, 8, 85, 16, 31, 32, 34, 65, 86, 79, 100, 25, 29, 81, 5, 7, 102, 22,
        30, 80, 101, 82, 68, 19, 21, 103, 39, 43, 89, 33, 44, 72, 66, 12, 36, 13, 93, 35, 87, 26, 9, 76, 27,
        10, 97, 70, 40, 23, 91, 83, 24, 74, 41, 104, 95, 78, 37, 106, 99, 38, 107, 108, 84, 105,
    ),
}


def slot(group, dz, k):
    return ("H", group * 9 + dz * 3 + k)


def far(dz, k):
    return ("F", dz * 2 + k)


def out_slot(group, dz, k):
    return ("O", (group - 1) * 9 + dz * 3 + k)


class Task:
    def __init__(self, kind, q, waits=(), waits_s=(), waits_r=(), sends=(), cost=0.0, args=(), role=None):
        self.kind = kind
        self.q = q
        self.waits = list(waits)
        self.waits_s = list(waits_s)
        self.waits_r = list(waits_r)
        self.sends = list(sends)
        self.cost = cost
        self.args = args
        self.role = role


def make_tasks(d_sizes, p_sizes, x_first=()):
    tasks = []
    for q in range(len(d_sizes)):
        c = slot(0, 1, OWN)
        tasks.append(Task("relay", q, sends=[
            (c, slot(0, 1, PAR), "partner", None),
            (c, slot(0, 0, OWN), "zp", None),
            (c, slot(0, 2, OWN), "zm", None),
            (c, far(1, PAR), "outer", "S"),
            (c, slot(1, 1, OWN), "sib", None),
        ]))
    for q in range(len(d_sizes)):
        c = slot(0, 1, PAR)
        tasks.append(Task("relay", q, [c], sends=[
            (c, slot(0, 1, CRS), "xd", None),
            (c, far(1, OWN), "outer", "S"),
            (c, slot(0, 0, PAR), "zp", None),
            (c, slot(0, 2, PAR), "zm", None),
            (c, slot(1, 1, PAR), "sib", None),
        ]))
        for dz in (0, 2):
            c = slot(0, dz, OWN)
            tasks.append(Task("relay", q, [c], sends=[
                (c, far(dz, PAR), "outer", "S"),
                (c, slot(1, dz, OWN), "sib", None),
            ]))
            c = slot(0, dz, PAR)
            sends = [(c, far(dz, OWN), "outer", "S")]
            if q not in x_first:
                sends.append((c, slot(0, dz, CRS), "xd", None))
            sends.append((c, slot(1, dz, PAR), "sib", None))
            tasks.append(Task("relay", q, [c], sends=sends))
        for dz in (1, 0, 2):
            c = slot(0, dz, CRS)
            sends = [(c, slot(1, dz, CRS), "sib", None)]
            if dz == 1 and q in x_first:
                sends = [(c, slot(0, 0, CRS), "zp", None), (c, slot(0, 2, CRS), "zm", None)] + sends
            tasks.append(Task("relay", q, [c], sends=sends))
        for k in (OWN, PAR):
            for dz in (1, 0, 2):
                c = far(dz, k)
                sends = []
                if dz == 1:
                    sends += [
                        (c, far(1, 1 - k), "partner", "R"),
                        (c, far(0, k), "zp", "S"),
                        (c, far(2, k), "zm", "S"),
                    ]
                if k == PAR:
                    sends.append((c, slot(2, dz, CRS), "sxd", None))
                sends.append((c, slot(2, dz, k), "sib", None))
                tasks.append(Task("relay", q, [c], sends=sends))
    tasks.append(Task("part", None, cost=3.2))
    for dz in (0, 2, 1):
        for k in (CRS, PAR, OWN):
            send = (out_slot(2, dz, k), ("RF", dz * 2 + k), "sib", None)
            if k == CRS:
                send = (out_slot(2, dz, k), ("XF", dz), "sxp", None)
            tasks.append(Task("sel", None, cost=0.03, args=(2, dz, k), sends=[send]))
    for k in (CRS, PAR, OWN):
        for dz in (0, 2, 1):
            tasks.append(Task("sel", None, cost=0.03, args=(1, dz, k), sends=[
                (out_slot(1, dz, k), ("RN", dz * 3 + k), "sib", None)]))
    for q, size in enumerate(p_sizes):
        unit = 0.14 * size / 16
        for dz in (0, 2):
            tasks.append(Task("add", q, [("RN", dz * 3 + CRS)], cost=unit, args=(("AX", dz), dz * 3 + CRS), sends=[
                (("AX", dz), ("ZX", dz // 2), "zm" if dz == 0 else "zp", None)]))
        tasks.append(Task("add", q, [("RN", 3 + CRS), ("ZX", 0), ("ZX", 1)], cost=unit * 1.5,
                          args=(("AX", 1), 3 + CRS), sends=[(("AX", 1), ("XN", 0), "xp", None)]))
        for dz in (0, 2, 1):
            for k in (PAR, OWN):
                here = ("AF", dz * 2 + k)
                waits = [("RF", dz * 2 + k)] + ([("XF", dz)] if k == PAR else [])
                if k == PAR:
                    tasks.append(Task("add", q, waits_s=waits, role="S", cost=unit, args=(here, None), sends=[
                        (here, ("IF", dz * 2 + 1 - k), "partner", "S")]))
                else:
                    tasks.append(Task("relay", q, waits_s=waits, role="S", sends=[
                        (waits[0], ("IF", dz * 2 + 1 - k), "partner", "S")]))
                tasks.append(Task("add", q, waits_r=waits + [("IF", dz * 2 + k)], role="R", cost=unit * 1.2,
                                  args=(here, None), sends=[(here, ("EN", dz * 2 + 1 - k), "outer", "R")]))
        for dz in (0, 2):
            for k in (PAR, OWN):
                tasks.append(Task("add", q, [("RN", dz * 3 + k)], [("EN", dz * 2 + k)], cost=unit * 1.2,
                                  args=(("AZ", dz + k), dz * 3 + k), sends=[
                    (("AZ", dz + k), ("ZN", dz + k), "zm" if dz == 0 else "zp", None)]))
        tasks.append(Task("add", q, [("RN", 3 + PAR), ("XN", 0), ("ZN", PAR), ("ZN", 2 + PAR)],
                          [("EN", 2 + PAR)], cost=unit * 1.6, args=(("AI", 0), 3 + PAR), sends=[
            (("AI", 0), ("IN", 0), "partner", None)]))
        tasks.append(Task("add", q, [("RN", 3 + OWN), ("ZN", OWN), ("ZN", 2 + OWN), ("IN", 0)],
                          [("EN", 2 + OWN)], cost=unit * 1.6, args=(None, 3 + OWN)))
    for q, size in enumerate(d_sizes):
        tasks.append(Task("forward", q, [("H", i) for i in range(27) if i != 3], cost=0.1 + 2.7 * size / 16))
    return tasks


TOGETHER, SEND_GROUPS = 18, 4

BUFFERS = {
    "H": (28, True), "F": (6, True),
    "O": (18, False), "AX": (3, False), "AF": (6, False), "AZ": (4, False), "AI": (1, False),
    "RN": (9, False), "RF": (6, False), "XN": (1, False), "XF": (3, False), "ZX": (2, False),
    "IF": (6, False), "EN": (6, False), "ZN": (4, False), "IN": (1, False),
}


def group_of(name, index):
    if name == "H":
        return ("near", index) if index < 9 else ("sibling",)
    if name in ("F", "IF"):
        return (name, index)
    if name in ("RF", "XF"):
        return ("far", index if name == "RF" else index * 2 + PAR)
    if name == "ZX":
        return ("cross", 1)
    if name in ("XN", "IN"):
        return ("centre", PAR if name == "XN" else OWN)
    if name == "ZN":
        return ("centre", index % 2)
    dz, k = divmod(index, 3 if name == "RN" else 2)
    if k == CRS:
        return ("cross", dz)
    return ("centre", k) if dz == 1 else ("outside", dz, k)


def arrivals_of():
    numbers = {}
    for name in ("H", "F", "RN", "RF", "IF"):
        for index in range(BUFFERS[name][0]):
            for q in range(len(chunks_of(name))):
                if name != "H" or index not in (3, 27):
                    numbers.setdefault((group_of(name, index), q), len(numbers))
    return numbers


def chunks_of(name):
    sizes = D_SIZES if BUFFERS[name][1] else P_SIZES
    return [(sum(sizes[:i]), size) for i, size in enumerate(sizes)]


def places(name, rows, columns):
    unit = (rows if BUFFERS[name][1] else columns) // 16
    return [(first * unit, size * unit) for first, size in chunks_of(name)]


def kernel(off_hbm, cnt_hbm, dens_ref, tile_hbm, out_ref, *scratch):
    names = list(BUFFERS)
    halo = scratch[:len(D_SIZES)]
    scratch = scratch[len(D_SIZES):]
    buf = dict(zip(names[1:], scratch[:len(names) - 1]))
    tiles = scratch[len(names) - 1:len(names) - 1 + len(D_SIZES)]
    (square, part, flip, picked, total, back, off_ref, cnt_ref, chosen,
     local_sem, tile_sem, send_sem, recv_sem) = scratch[len(names) - 1 + len(D_SIZES):]
    gx, gy, gz = lax.axis_index("gx"), lax.axis_index("gy"), lax.axis_index("gz")
    nx, ny, nz = lax.axis_size("gx"), lax.axis_size("gy"), lax.axis_size("gz")
    b, c = lax.rem(gx, 2), lax.rem(gy, 2)
    xd = lax.rem(gx + 2 - 4 * b + nx, nx)
    xp = lax.rem(gx - 2 + 4 * b + nx, nx)
    sib = gy + 1 - 2 * c
    outer_x = lax.rem(gx + 1 - 2 * b + nx, nx)
    where_to = {
        "partner": (outer_x, gy, gz),
        "outer": (outer_x, lax.rem(gy - 2 + 4 * b + ny, ny), gz),
        "sib": (gx, sib, gz),
        "xd": (xd, gy, gz), "xp": (xp, gy, gz),
        "sxd": (xd, sib, gz), "sxp": (xp, sib, gz),
        "zp": (gx, gy, lax.rem(gz + 1, nz)),
        "zm": (gx, gy, lax.rem(gz + nz - 1, nz)),
    }
    rows, columns = total.shape
    slots = off_ref.shape[-1]
    d_places = places("H", rows, columns)

    barrier = pltpu.get_barrier_semaphore()
    for target in where_to.values():
        pl.semaphore_signal(barrier, inc=1, device_id=target, device_id_type=MESH)
    density_copies = []
    for q, (first, size) in enumerate(d_places):
        copy = pltpu.make_async_copy(
            dens_ref.at[0, 0, 0, pl.ds(first, size)], halo[q].at[3], local_sem.at[slots + q])
        copy.start()
        density_copies.append(copy)
    index_copies = [
        pltpu.make_async_copy(off_hbm, off_ref, local_sem.at[slots + len(d_places)]),
        pltpu.make_async_copy(cnt_hbm, cnt_ref, local_sem.at[slots + len(d_places) + 1]),
    ]
    for copy in index_copies:
        copy.start()

    def tile_copy(s, q):
        first, size = d_places[q]
        return pltpu.make_async_copy(
            tile_hbm.at[0, 0, 0, s, :, pl.ds(first, size)], tiles[q].at[:, pl.ds(s * size, size)],
            tile_sem.at[q])

    for s in range(slots):
        pltpu.make_async_copy(tile_hbm.at[0, 0, 0, s], square.at[s], local_sem.at[s]).start()

    def piece(name, index, q):
        if name == "H":
            return halo[q].at[index]
        first, size = places(name, rows, columns)[q]
        return buf[name].at[index, pl.ds(first, size)]

    numbers = arrivals_of()

    def arrival(name, index, q):
        return recv_sem.at[numbers[group_of(name, index), q]]

    def wait_blocks(name, n, q, semaphore):
        if BUFFERS[name][1]:
            ref = halo[q].at[pl.ds(0, n)]
        else:
            first, size = places(name, rows, columns)[q]
            ref = buf["O"].at[pl.ds(0, n), pl.ds(first, size)]
        pltpu.make_async_copy(ref, ref, semaphore).wait()

    def add(target, q, terms, own):
        first, size = places("AF", rows, columns)[q]
        strip = 32

        @pl.loop(0, size // strip)
        def _(i):
            span = pl.ds(pl.multiple_of(first + i * strip, strip), strip)
            value = None
            if own is not None:
                value = part[chosen[own], span].astype(jnp.float32)
            for name, index in terms:
                term = buf[name][index, span].astype(jnp.float32)
                value = term if value is None else value + term
            if target is None:
                back[span] = value
            else:
                buf[target[0]][target[1], span] = value.astype(jnp.bfloat16)

    def find_tiles():
        live = cnt_ref[0, 0, 0]
        home = []
        for s in range(slots):
            code = off_ref[0, 0, 0, s]
            dx, dy, dz = lax.div(code, 9), lax.rem(lax.div(code, 3), 3), lax.rem(code, 3)
            k = jnp.where(dx == 1, OWN, jnp.where(dx == 2 - 2 * b, PAR, CRS))
            group = jnp.where(dy == 1, 0, jnp.where(dy == 2 - 2 * c, 1, 2))
            home.append(jnp.where(s < live, group * 9 + dz * 3 + k, 27))
            chosen[27 + s] = home[s]

        @pl.loop(0, 27)
        def _(h):
            index = jnp.int32(slots)
            for s in range(slots):
                index = jnp.where(home[s] == h, s, index)
            chosen[h] = index

    def partials():
        for q, (first, size) in enumerate(d_places):
            flip[:, first:first + size] = halo[q][3].T
            halo[q][27] = jnp.zeros((size, columns), jnp.bfloat16)
        part[slots] = jnp.zeros((columns, rows), jnp.bfloat16)
        total[...] = jnp.zeros_like(total)
        for copy in index_copies:
            copy.wait()
        find_tiles()

        @pl.loop(0, slots)
        def _(s):
            pltpu.make_async_copy(tile_hbm.at[0, 0, 0, s], square.at[s], local_sem.at[s]).wait()
            part[s] = jnp.dot(flip[...], square[s], preferred_element_type=jnp.float32).astype(jnp.bfloat16)

        for s in range(slots):
            for q in range(len(d_places)):
                tile_copy(s, q).start()

    def forward(q):
        size = d_places[q][1]
        pltpu.make_async_copy(tiles[q], tiles[q], tile_sem.at[q]).wait()
        for s in range(slots):
            picked[s * size:(s + 1) * size] = halo[q][chosen[27 + s]]
        total[...] += jnp.dot(tiles[q][...], picked[:slots * size], preferred_element_type=jnp.float32)

    tasks = make_tasks(D_SIZES, P_SIZES, X_FIRST)

    def send_number(straight, q, n):
        return (q if straight else len(D_SIZES) + q) * SEND_GROUPS + n // TOGETHER

    def run(role):
        waited = set()
        sent = {}
        for number in ORDER[role]:
            task = tasks[number]
            keys = task.waits + (task.waits_s if role == "S" else task.waits_r)
            groups = {}
            for key in keys:
                if (key, task.q) not in waited:
                    waited.add((key, task.q))
                    groups.setdefault(group_of(*key), []).append(key)
            for members in groups.values():
                wait_blocks(members[0][0], len(members), task.q, arrival(*members[0], task.q))
            if task.kind == "part":
                partials()
            elif task.kind == "forward":
                forward(task.q)
            elif task.kind == "sel":
                group, dz, k = task.args
                buf["O"][(group - 1) * 9 + dz * 3 + k] = part[chosen[group * 9 + dz * 3 + k]]
            elif task.kind == "add":
                add(task.args[0], task.q, keys, task.args[1])
            elif number < len(D_SIZES):
                density_copies[number].wait()
            for source, target, to, only in task.sends:
                if only in (None, role):
                    for q in range(len(P_SIZES)) if task.q is None else [task.q]:
                        straight = BUFFERS[target[0]][1]
                        kind = (straight, q)
                        sent[kind] = sent.get(kind, 0) + 1
                        pltpu.make_async_remote_copy(
                            src_ref=piece(source[0], source[1], q),
                            dst_ref=piece(target[0], target[1], q),
                            send_sem=send_sem.at[send_number(*kind, sent[kind] - 1)],
                            recv_sem=arrival(target[0], target[1], q),
                            device_id=where_to[to],
                            device_id_type=MESH,
                        ).start()
        out_ref[0, 0, 0] = (total[...] + back[...].T).astype(out_ref.dtype)
        for (straight, q), n in sent.items():
            for first in range(0, n, TOGETHER):
                wait_blocks("H" if straight else "O", min(TOGETHER, n - first), q,
                            send_sem.at[send_number(straight, q, first)])

    pl.semaphore_wait(barrier, len(where_to))
    pl.when(b == c)(functools.partial(run, "S"))
    pl.when(b != c)(functools.partial(run, "R"))


def local(density, integrals, offsets, counts):
    rows, columns = density.shape[3:]
    slots = integrals.shape[3]
    sends = (len(D_SIZES) + len(P_SIZES)) * SEND_GROUPS
    arrivals = len(arrivals_of())
    scratch = [pltpu.VMEM((BUFFERS["H"][0], size, columns), jnp.bfloat16) for _, size in places("H", rows, columns)]
    scratch += [
        pltpu.VMEM((n, rows, columns) if straight else (n, columns, rows), jnp.bfloat16)
        for name, (n, straight) in BUFFERS.items() if name != "H"
    ]
    scratch += [
        pltpu.VMEM((rows, slots * size), jnp.bfloat16) for _, size in places("H", rows, columns)
    ]
    scratch += [
        pltpu.VMEM((slots, rows, rows), jnp.bfloat16),
        pltpu.VMEM((slots + 1, columns, rows), jnp.bfloat16),
        pltpu.VMEM((columns, rows), jnp.bfloat16),
        pltpu.VMEM((slots * max(size for _, size in places("H", rows, columns)), columns), jnp.bfloat16),
        pltpu.VMEM((rows, columns), jnp.float32),
        pltpu.VMEM((columns, rows), jnp.float32),
        pltpu.SMEM(offsets.shape, jnp.int32),
        pltpu.SMEM(counts.shape, jnp.int32),
        pltpu.SMEM((27 + slots,), jnp.int32),
        pltpu.SemaphoreType.DMA((slots + len(D_SIZES) + 2,)),
        pltpu.SemaphoreType.DMA((len(D_SIZES),)),
        pltpu.SemaphoreType.DMA((sends,)),
        pltpu.SemaphoreType.DMA((arrivals,)),
    ]
    return pl.pallas_call(
        kernel,
        out_shape=jax.ShapeDtypeStruct(density.shape, density.dtype),
        in_specs=[
            pl.BlockSpec(memory_space=pl.ANY),
            pl.BlockSpec(memory_space=pl.ANY),
            pl.BlockSpec(memory_space=pl.ANY),
            pl.BlockSpec(memory_space=pl.ANY),
        ],
        out_specs=pl.BlockSpec(memory_space=pltpu.VMEM),
        scratch_shapes=scratch,
        compiler_params=pltpu.CompilerParams(
            collective_id=0, has_side_effects=True, vmem_limit_bytes=VMEM_LIMIT
        ),
    )(offsets, counts, density, integrals)


def solution(mesh):
    return jax.shard_map(
        local,
        mesh=mesh,
        in_specs=(
            P("gx", "gy", "gz", None, None),
            P("gx", "gy", "gz", None, None, None),
            P("gx", "gy", "gz", None),
            P("gx", "gy", "gz"),
        ),
        out_specs=P("gx", "gy", "gz", None, None),
        check_vma=False,
    )
```

```python
import functools

import jax
import jax.numpy as jnp
from jax import lax
from jax.experimental import pallas as pl
from jax.experimental.pallas import tpu as pltpu
from jax.sharding import PartitionSpec as P

MESH = pl.DeviceIdType.MESH
OWN, PAR, CRS = 0, 1, 2
VMEM_LIMIT = 56164352
D_SIZES = (4, 4, 4, 4)
P_SIZES = (8, 4, 4)
X_FIRST, Z_FAR, X_NEAR = ((2,), (0,), (0,))
ORDER = {
    "S": (
        0, 1, 2, 3, 60, 61, 4, 5, 7, 62, 63, 64, 65, 66, 67, 68, 69, 70, 71, 72, 73, 74, 75, 76, 77, 78, 18,
        19, 21, 84, 105, 126, 32, 33, 35, 88, 109, 130, 9, 92, 113, 134, 46, 47, 49, 79, 100, 121, 80, 23,
        82, 101, 122, 81, 6, 8, 12, 103, 37, 20, 22, 26, 124, 51, 34, 36, 40, 10, 48, 50, 54, 86, 11, 102,
        15, 107, 24, 95, 123, 29, 128, 25, 116, 13, 14, 43, 52, 137, 38, 39, 57, 90, 53, 27, 28, 111, 97,
        41, 42, 118, 132, 139, 55, 56, 16, 17, 30, 142, 44, 94, 115, 136, 58, 31, 96, 144, 117, 143, 45,
        138, 59, 98, 120, 119, 140, 145, 99, 141,
    ),
    "R": (
        0, 1, 2, 3, 60, 15, 61, 4, 5, 7, 29, 62, 63, 64, 65, 66, 67, 68, 69, 70, 71, 72, 73, 74, 43, 75, 76,
        77, 78, 18, 19, 21, 57, 12, 32, 33, 35, 79, 100, 46, 47, 49, 121, 80, 9, 101, 26, 30, 122, 81, 31,
        115, 136, 16, 17, 117, 138, 95, 116, 40, 44, 137, 83, 6, 8, 97, 118, 139, 45, 104, 20, 22, 23, 54,
        58, 125, 13, 14, 59, 34, 36, 37, 27, 87, 48, 28, 108, 50, 102, 51, 41, 129, 123, 42, 91, 55, 112,
        56, 133, 85, 106, 127, 10, 94, 11, 89, 110, 131, 96, 93, 38, 39, 24, 142, 114, 135, 25, 119, 98, 52,
        140, 53, 143, 144, 145, 99, 120, 141,
    ),
}


def slot(group, dz, k):
    return ("H", group * 9 + dz * 3 + k)


def far(dz, k):
    return ("F", dz * 2 + k)


def out_slot(group, dz, k):
    return ("O", (group - 1) * 9 + dz * 3 + k)


class Task:
    def __init__(self, kind, q, waits=(), waits_s=(), waits_r=(), sends=(), cost=0.0, args=(), role=None):
        self.kind = kind
        self.q = q
        self.waits = list(waits)
        self.waits_s = list(waits_s)
        self.waits_r = list(waits_r)
        self.sends = list(sends)
        self.cost = cost
        self.args = args
        self.role = role


def make_tasks(d_sizes, p_sizes, x_first=(), z_far=(), x_near=()):
    tasks = []
    for q in range(len(d_sizes)):
        c = slot(0, 1, OWN)
        tasks.append(Task("relay", q, sends=[
            (c, slot(0, 1, PAR), "partner", None),
            (c, slot(0, 0, OWN), "zp", None),
            (c, slot(0, 2, OWN), "zm", None),
            (c, far(1, PAR), "outer", "S"),
            (c, slot(1, 1, OWN), "sib", None),
        ]))
    for q in range(len(d_sizes)):
        c = slot(0, 1, PAR)
        tasks.append(Task("relay", q, [c], sends=[
            (c, slot(0, 1, CRS), "xd", None),
            (c, far(1, OWN), "outer", "S"),
            (c, slot(0, 0, PAR), "zp", None),
            (c, slot(0, 2, PAR), "zm", None),
            (c, slot(1, 1, PAR), "sib", None),
        ]))
        for dz in (0, 2):
            c = slot(0, dz, OWN)
            across = [] if q in z_far else [(c, far(dz, PAR), "outer", "S")]
            tasks.append(Task("relay", q, [c], sends=across + [(c, slot(1, dz, OWN), "sib", None)]))
            c = slot(0, dz, PAR)
            sends = [] if q in z_far else [(c, far(dz, OWN), "outer", "S")]
            if q not in x_first:
                sends.append((c, slot(0, dz, CRS), "xd", None))
            sends.append((c, slot(1, dz, PAR), "sib", None))
            tasks.append(Task("relay", q, [c], sends=sends))
        for dz in (1, 0, 2):
            c = slot(0, dz, CRS)
            sends = [(c, slot(1, dz, CRS), "sib", None)]
            if dz == 1 and q in x_first:
                sends = [(c, slot(0, 0, CRS), "zp", None), (c, slot(0, 2, CRS), "zm", None)] + sends
            tasks.append(Task("relay", q, [c], sends=sends))
        for k in (OWN, PAR):
            for dz in (1, 0, 2):
                c = far(dz, k)
                sends = []
                if dz == 1:
                    sends += [
                        (c, far(1, 1 - k), "partner", "R"),
                        (c, far(0, k), "zp", None if q in z_far else "S"),
                        (c, far(2, k), "zm", None if q in z_far else "S"),
                    ]
                if k == PAR:
                    sends.append((c, slot(2, dz, CRS), "sxd", None))
                sends.append((c, slot(2, dz, k), "sib", None))
                tasks.append(Task("relay", q, [c], sends=sends))
    tasks.append(Task("part", None, cost=3.2))
    for dz in (0, 2, 1):
        for k in (CRS, PAR, OWN):
            send = (out_slot(2, dz, k), ("RF", dz * 2 + k), "sib", None)
            if k == CRS:
                send = (out_slot(2, dz, k), ("XF", dz), "sxp", None)
            tasks.append(Task("sel", None, cost=0.03, args=(2, dz, k), sends=[send]))
    for k in (CRS, PAR, OWN):
        for dz in (0, 2, 1):
            tasks.append(Task("sel", None, cost=0.03, args=(1, dz, k), sends=[
                (out_slot(1, dz, k), ("RN", dz * 3 + k), "sib", None)]))
    for q, size in enumerate(p_sizes):
        unit = 0.14 * size / 16
        for dz in (0, 2):
            send = (("AX", dz), ("ZX", dz // 2), "zm" if dz == 0 else "zp", None)
            if q in x_near:
                send = (("AX", dz), ("XN", dz), "xp", None)
            tasks.append(Task("add", q, [("RN", dz * 3 + CRS)], cost=unit, args=(("AX", dz), dz * 3 + CRS),
                              sends=[send]))
        waits = [("RN", 3 + CRS)] + ([] if q in x_near else [("ZX", 0), ("ZX", 1)])
        tasks.append(Task("add", q, waits, cost=unit * 1.5,
                          args=(("AX", 1), 3 + CRS), sends=[(("AX", 1), ("XN", 1), "xp", None)]))
        for dz in (0, 2, 1):
            for k in (PAR, OWN):
                here = ("AF", dz * 2 + k)
                waits = [("RF", dz * 2 + k)] + ([("XF", dz)] if k == PAR else [])
                if k == PAR:
                    tasks.append(Task("add", q, waits_s=waits, role="S", cost=unit, args=(here, None), sends=[
                        (here, ("IF", dz * 2 + 1 - k), "partner", "S")]))
                else:
                    tasks.append(Task("relay", q, waits_s=waits, role="S", sends=[
                        (waits[0], ("IF", dz * 2 + 1 - k), "partner", "S")]))
                tasks.append(Task("add", q, waits_r=waits + [("IF", dz * 2 + k)], role="R", cost=unit * 1.2,
                                  args=(here, None), sends=[(here, ("EN", dz * 2 + 1 - k), "outer", "R")]))
        for dz in (0, 2):
            for k in (PAR, OWN):
                waits = [("RN", dz * 3 + k)] + ([("XN", dz)] if k == PAR and q in x_near else [])
                tasks.append(Task("add", q, waits, [("EN", dz * 2 + k)], cost=unit * 1.2,
                                  args=(("AZ", dz + k), dz * 3 + k), sends=[
                    (("AZ", dz + k), ("ZN", dz + k), "zm" if dz == 0 else "zp", None)]))
        tasks.append(Task("add", q, [("RN", 3 + PAR), ("XN", 1), ("ZN", PAR), ("ZN", 2 + PAR)],
                          [("EN", 2 + PAR)], cost=unit * 1.6, args=(("AI", 0), 3 + PAR), sends=[
            (("AI", 0), ("IN", 0), "partner", None)]))
        tasks.append(Task("add", q, [("RN", 3 + OWN), ("ZN", OWN), ("ZN", 2 + OWN), ("IN", 0)],
                          [("EN", 2 + OWN)], cost=unit * 1.6, args=(None, 3 + OWN)))
    for q, size in enumerate(d_sizes):
        tasks.append(Task("forward", q, [("H", i) for i in range(27) if i != 3], cost=0.1 + 2.7 * size / 16))
    return tasks


TOGETHER, SEND_GROUPS = 18, 4

BUFFERS = {
    "H": (28, True), "F": (6, True),
    "O": (18, False), "AX": (3, False), "AF": (6, False), "AZ": (4, False), "AI": (1, False),
    "RN": (9, False), "RF": (6, False), "XN": (3, False), "XF": (3, False), "ZX": (2, False),
    "IF": (6, False), "EN": (6, False), "ZN": (4, False), "IN": (1, False),
}


def group_of(name, index):
    if name == "H":
        return ("near", index) if index < 9 else ("sibling",)
    if name in ("F", "IF"):
        return (name, index)
    if name in ("RF", "XF"):
        return ("far", index if name == "RF" else index * 2 + PAR)
    if name == "ZX":
        return ("cross", 1)
    if name == "XN":
        return ("centre", PAR) if index == 1 else ("outside", index, PAR)
    if name == "IN":
        return ("centre", OWN)
    if name == "ZN":
        return ("centre", index % 2)
    dz, k = divmod(index, 3 if name == "RN" else 2)
    if k == CRS:
        return ("cross", dz)
    return ("centre", k) if dz == 1 else ("outside", dz, k)


def arrivals_of():
    numbers = {}
    for name in ("H", "F", "RN", "RF", "IF"):
        for index in range(BUFFERS[name][0]):
            for q in range(len(chunks_of(name))):
                if name != "H" or index not in (3, 27):
                    numbers.setdefault((group_of(name, index), q), len(numbers))
    return numbers


def chunks_of(name):
    sizes = D_SIZES if BUFFERS[name][1] else P_SIZES
    return [(sum(sizes[:i]), size) for i, size in enumerate(sizes)]


def places(name, rows, columns):
    unit = (rows if BUFFERS[name][1] else columns) // 16
    return [(first * unit, size * unit) for first, size in chunks_of(name)]


def kernel(off_hbm, cnt_hbm, dens_ref, tile_hbm, out_ref, *scratch):
    names = list(BUFFERS)
    halo = scratch[:len(D_SIZES)]
    scratch = scratch[len(D_SIZES):]
    buf = dict(zip(names[1:], scratch[:len(names) - 1]))
    tiles = scratch[len(names) - 1:len(names) - 1 + len(D_SIZES)]
    (square, part, flip, picked, total, back, off_ref, cnt_ref, chosen,
     local_sem, tile_sem, send_sem, recv_sem) = scratch[len(names) - 1 + len(D_SIZES):]
    gx, gy, gz = lax.axis_index("gx"), lax.axis_index("gy"), lax.axis_index("gz")
    nx, ny, nz = lax.axis_size("gx"), lax.axis_size("gy"), lax.axis_size("gz")
    b, c = lax.rem(gx, 2), lax.rem(gy, 2)
    xd = lax.rem(gx + 2 - 4 * b + nx, nx)
    xp = lax.rem(gx - 2 + 4 * b + nx, nx)
    sib = gy + 1 - 2 * c
    outer_x = lax.rem(gx + 1 - 2 * b + nx, nx)
    where_to = {
        "partner": (outer_x, gy, gz),
        "outer": (outer_x, lax.rem(gy - 2 + 4 * b + ny, ny), gz),
        "sib": (gx, sib, gz),
        "xd": (xd, gy, gz), "xp": (xp, gy, gz),
        "sxd": (xd, sib, gz), "sxp": (xp, sib, gz),
        "zp": (gx, gy, lax.rem(gz + 1, nz)),
        "zm": (gx, gy, lax.rem(gz + nz - 1, nz)),
    }
    rows, columns = total.shape
    slots = off_ref.shape[-1]
    d_places = places("H", rows, columns)

    barrier = pltpu.get_barrier_semaphore()
    for target in where_to.values():
        pl.semaphore_signal(barrier, inc=1, device_id=target, device_id_type=MESH)
    density_copies = []
    for q, (first, size) in enumerate(d_places):
        copy = pltpu.make_async_copy(
            dens_ref.at[0, 0, 0, pl.ds(first, size)], halo[q].at[3], local_sem.at[slots + q])
        copy.start()
        density_copies.append(copy)
    index_copies = [
        pltpu.make_async_copy(off_hbm, off_ref, local_sem.at[slots + len(d_places)]),
        pltpu.make_async_copy(cnt_hbm, cnt_ref, local_sem.at[slots + len(d_places) + 1]),
    ]
    for copy in index_copies:
        copy.start()

    def tile_copy(s, q):
        first, size = d_places[q]
        return pltpu.make_async_copy(
            tile_hbm.at[0, 0, 0, s, :, pl.ds(first, size)], tiles[q].at[:, pl.ds(s * size, size)],
            tile_sem.at[q])

    for s in range(slots):
        pltpu.make_async_copy(tile_hbm.at[0, 0, 0, s], square.at[s], local_sem.at[s]).start()

    def piece(name, index, q):
        if name == "H":
            return halo[q].at[index]
        first, size = places(name, rows, columns)[q]
        return buf[name].at[index, pl.ds(first, size)]

    numbers = arrivals_of()

    def arrival(name, index, q):
        return recv_sem.at[numbers[group_of(name, index), q]]

    def wait_blocks(name, n, q, semaphore):
        if BUFFERS[name][1]:
            ref = halo[q].at[pl.ds(0, n)]
        else:
            first, size = places(name, rows, columns)[q]
            ref = buf["O"].at[pl.ds(0, n), pl.ds(first, size)]
        pltpu.make_async_copy(ref, ref, semaphore).wait()

    def add(target, q, terms, own):
        first, size = places("AF", rows, columns)[q]
        strip = 32

        @pl.loop(0, size // strip)
        def _(i):
            span = pl.ds(pl.multiple_of(first + i * strip, strip), strip)
            value = None
            if own is not None:
                value = part[chosen[own], span].astype(jnp.float32)
            for name, index in terms:
                term = buf[name][index, span].astype(jnp.float32)
                value = term if value is None else value + term
            if target is None:
                back[span] = value
            else:
                buf[target[0]][target[1], span] = value.astype(jnp.bfloat16)

    def find_tiles():
        live = cnt_ref[0, 0, 0]
        home = []
        for s in range(slots):
            code = off_ref[0, 0, 0, s]
            dx, dy, dz = lax.div(code, 9), lax.rem(lax.div(code, 3), 3), lax.rem(code, 3)
            k = jnp.where(dx == 1, OWN, jnp.where(dx == 2 - 2 * b, PAR, CRS))
            group = jnp.where(dy == 1, 0, jnp.where(dy == 2 - 2 * c, 1, 2))
            home.append(jnp.where(s < live, group * 9 + dz * 3 + k, 27))
            chosen[27 + s] = home[s]

        @pl.loop(0, 27)
        def _(h):
            index = jnp.int32(slots)
            for s in range(slots):
                index = jnp.where(home[s] == h, s, index)
            chosen[h] = index

    def partials():
        for q, (first, size) in enumerate(d_places):
            flip[:, first:first + size] = halo[q][3].T
            halo[q][27] = jnp.zeros((size, columns), jnp.bfloat16)
        part[slots] = jnp.zeros((columns, rows), jnp.bfloat16)
        total[...] = jnp.zeros_like(total)
        for copy in index_copies:
            copy.wait()
        find_tiles()

        @pl.loop(0, slots)
        def _(s):
            pltpu.make_async_copy(tile_hbm.at[0, 0, 0, s], square.at[s], local_sem.at[s]).wait()
            part[s] = jnp.dot(flip[...], square[s], preferred_element_type=jnp.float32).astype(jnp.bfloat16)

        for s in range(slots):
            for q in range(len(d_places)):
                tile_copy(s, q).start()

    def forward(q):
        size = d_places[q][1]
        pltpu.make_async_copy(tiles[q], tiles[q], tile_sem.at[q]).wait()
        for s in range(slots):
            picked[s * size:(s + 1) * size] = halo[q][chosen[27 + s]]
        total[...] += jnp.dot(tiles[q][...], picked[:slots * size], preferred_element_type=jnp.float32)

    tasks = make_tasks(D_SIZES, P_SIZES, X_FIRST, Z_FAR, X_NEAR)

    def send_number(straight, q, n):
        return (q if straight else len(D_SIZES) + q) * SEND_GROUPS + n // TOGETHER

    def run(role):
        waited = set()
        sent = {}
        for number in ORDER[role]:
            task = tasks[number]
            keys = task.waits + (task.waits_s if role == "S" else task.waits_r)
            groups = {}
            for key in keys:
                if (key, task.q) not in waited:
                    waited.add((key, task.q))
                    groups.setdefault(group_of(*key), []).append(key)
            for members in groups.values():
                wait_blocks(members[0][0], len(members), task.q, arrival(*members[0], task.q))
            if task.kind == "part":
                partials()
            elif task.kind == "forward":
                forward(task.q)
            elif task.kind == "sel":
                group, dz, k = task.args
                buf["O"][(group - 1) * 9 + dz * 3 + k] = part[chosen[group * 9 + dz * 3 + k]]
            elif task.kind == "add":
                add(task.args[0], task.q, keys, task.args[1])
            elif number < len(D_SIZES):
                density_copies[number].wait()
            for source, target, to, only in task.sends:
                if only in (None, role):
                    for q in range(len(P_SIZES)) if task.q is None else [task.q]:
                        straight = BUFFERS[target[0]][1]
                        kind = (straight, q)
                        sent[kind] = sent.get(kind, 0) + 1
                        pltpu.make_async_remote_copy(
                            src_ref=piece(source[0], source[1], q),
                            dst_ref=piece(target[0], target[1], q),
                            send_sem=send_sem.at[send_number(*kind, sent[kind] - 1)],
                            recv_sem=arrival(target[0], target[1], q),
                            device_id=where_to[to],
                            device_id_type=MESH,
                        ).start()
        out_ref[0, 0, 0] = (total[...] + back[...].T).astype(out_ref.dtype)
        for (straight, q), n in sent.items():
            for first in range(0, n, TOGETHER):
                wait_blocks("H" if straight else "O", min(TOGETHER, n - first), q,
                            send_sem.at[send_number(straight, q, first)])

    pl.semaphore_wait(barrier, len(where_to))
    pl.when(b == c)(functools.partial(run, "S"))
    pl.when(b != c)(functools.partial(run, "R"))


def local(density, integrals, offsets, counts):
    rows, columns = density.shape[3:]
    slots = integrals.shape[3]
    sends = (len(D_SIZES) + len(P_SIZES)) * SEND_GROUPS
    arrivals = len(arrivals_of())
    scratch = [pltpu.VMEM((BUFFERS["H"][0], size, columns), jnp.bfloat16) for _, size in places("H", rows, columns)]
    scratch += [
        pltpu.VMEM((n, rows, columns) if straight else (n, columns, rows), jnp.bfloat16)
        for name, (n, straight) in BUFFERS.items() if name != "H"
    ]
    scratch += [
        pltpu.VMEM((rows, slots * size), jnp.bfloat16) for _, size in places("H", rows, columns)
    ]
    scratch += [
        pltpu.VMEM((slots, rows, rows), jnp.bfloat16),
        pltpu.VMEM((slots + 1, columns, rows), jnp.bfloat16),
        pltpu.VMEM((columns, rows), jnp.bfloat16),
        pltpu.VMEM((slots * max(size for _, size in places("H", rows, columns)), columns), jnp.bfloat16),
        pltpu.VMEM((rows, columns), jnp.float32),
        pltpu.VMEM((columns, rows), jnp.float32),
        pltpu.SMEM(offsets.shape, jnp.int32),
        pltpu.SMEM(counts.shape, jnp.int32),
        pltpu.SMEM((27 + slots,), jnp.int32),
        pltpu.SemaphoreType.DMA((slots + len(D_SIZES) + 2,)),
        pltpu.SemaphoreType.DMA((len(D_SIZES),)),
        pltpu.SemaphoreType.DMA((sends,)),
        pltpu.SemaphoreType.DMA((arrivals,)),
    ]
    return pl.pallas_call(
        kernel,
        out_shape=jax.ShapeDtypeStruct(density.shape, density.dtype),
        in_specs=[
            pl.BlockSpec(memory_space=pl.ANY),
            pl.BlockSpec(memory_space=pl.ANY),
            pl.BlockSpec(memory_space=pl.ANY),
            pl.BlockSpec(memory_space=pl.ANY),
        ],
        out_specs=pl.BlockSpec(memory_space=pltpu.VMEM),
        scratch_shapes=scratch,
        compiler_params=pltpu.CompilerParams(
            collective_id=0, has_side_effects=True, vmem_limit_bytes=VMEM_LIMIT
        ),
    )(offsets, counts, density, integrals)


def solution(mesh):
    return jax.shard_map(
        local,
        mesh=mesh,
        in_specs=(
            P("gx", "gy", "gz", None, None),
            P("gx", "gy", "gz", None, None, None),
            P("gx", "gy", "gz", None),
            P("gx", "gy", "gz"),
        ),
        out_specs=P("gx", "gy", "gz", None, None),
        check_vma=False,
    )
```

```python
import functools

import jax
import jax.numpy as jnp
from jax import lax
from jax.experimental import pallas as pl
from jax.experimental.pallas import tpu as pltpu
from jax.sharding import PartitionSpec as P

MESH = pl.DeviceIdType.MESH
OWN, PAR, CRS = 0, 1, 2
VMEM_LIMIT = 56164352
D_SIZES = (4, 4, 4, 4)
P_SIZES = (8, 4, 4)
X_FIRST, Z_FAR, X_NEAR = ((2,), (0,), (0,))
ORDER = {
    "S": (
        0, 1, 2, 3, 60, 61, 4, 5, 7, 62, 63, 64, 65, 66, 67, 68, 69, 70, 71, 72, 73, 74, 75, 76, 77, 78, 18,
        19, 21, 84, 105, 126, 32, 33, 35, 88, 109, 130, 9, 92, 113, 134, 46, 47, 49, 79, 100, 121, 80, 23,
        82, 101, 122, 81, 6, 8, 12, 103, 37, 20, 22, 26, 124, 51, 34, 36, 40, 10, 48, 50, 54, 86, 11, 102,
        15, 107, 24, 95, 123, 29, 128, 25, 116, 13, 14, 43, 52, 137, 38, 39, 57, 90, 53, 27, 28, 111, 97,
        41, 42, 118, 132, 139, 55, 56, 16, 17, 30, 142, 44, 94, 115, 136, 58, 31, 96, 144, 117, 143, 45,
        138, 59, 98, 120, 119, 140, 145, 99, 141,
    ),
    "R": (
        0, 1, 2, 3, 60, 15, 61, 4, 5, 7, 29, 62, 63, 64, 65, 66, 67, 68, 69, 70, 71, 72, 73, 74, 43, 75, 76,
        77, 78, 18, 19, 21, 57, 12, 32, 33, 35, 79, 100, 46, 47, 49, 121, 80, 9, 101, 26, 30, 122, 81, 31,
        115, 136, 16, 17, 117, 138, 95, 116, 40, 44, 137, 83, 6, 8, 97, 118, 139, 45, 104, 20, 22, 23, 54,
        58, 125, 13, 14, 59, 34, 36, 37, 27, 87, 48, 28, 108, 50, 102, 51, 41, 129, 123, 42, 91, 55, 112,
        56, 133, 85, 106, 127, 10, 94, 11, 89, 110, 131, 96, 93, 38, 39, 24, 142, 114, 135, 25, 119, 98, 52,
        140, 53, 143, 144, 145, 99, 120, 141,
    ),
}


def slot(group, dz, k):
    return ("H", group * 9 + dz * 3 + k)


def far(dz, k):
    return ("F", dz * 2 + k)


def out_slot(group, dz, k):
    return ("O", (group - 1) * 9 + dz * 3 + k)


class Task:
    def __init__(self, kind, q, waits=(), waits_s=(), waits_r=(), sends=(), cost=0.0, args=(), role=None):
        self.kind = kind
        self.q = q
        self.waits = list(waits)
        self.waits_s = list(waits_s)
        self.waits_r = list(waits_r)
        self.sends = list(sends)
        self.cost = cost
        self.args = args
        self.role = role


def make_tasks(d_sizes, p_sizes, x_first=(), z_far=(), x_near=()):
    tasks = []
    for q in range(len(d_sizes)):
        c = slot(0, 1, OWN)
        tasks.append(Task("relay", q, sends=[
            (c, slot(0, 1, PAR), "partner", None),
            (c, slot(0, 0, OWN), "zp", None),
            (c, slot(0, 2, OWN), "zm", None),
            (c, far(1, PAR), "outer", "S"),
            (c, slot(1, 1, OWN), "sib", None),
        ]))
    for q in range(len(d_sizes)):
        c = slot(0, 1, PAR)
        tasks.append(Task("relay", q, [c], sends=[
            (c, slot(0, 1, CRS), "xd", None),
            (c, far(1, OWN), "outer", "S"),
            (c, slot(0, 0, PAR), "zp", None),
            (c, slot(0, 2, PAR), "zm", None),
            (c, slot(1, 1, PAR), "sib", None),
        ]))
        for dz in (0, 2):
            c = slot(0, dz, OWN)
            across = [] if q in z_far else [(c, far(dz, PAR), "outer", "S")]
            tasks.append(Task("relay", q, [c], sends=across + [(c, slot(1, dz, OWN), "sib", None)]))
            c = slot(0, dz, PAR)
            sends = [] if q in z_far else [(c, far(dz, OWN), "outer", "S")]
            if q not in x_first:
                sends.append((c, slot(0, dz, CRS), "xd", None))
            sends.append((c, slot(1, dz, PAR), "sib", None))
            tasks.append(Task("relay", q, [c], sends=sends))
        for dz in (1, 0, 2):
            c = slot(0, dz, CRS)
            sends = [(c, slot(1, dz, CRS), "sib", None)]
            if dz == 1 and q in x_first:
                sends = [(c, slot(0, 0, CRS), "zp", None), (c, slot(0, 2, CRS), "zm", None)] + sends
            tasks.append(Task("relay", q, [c], sends=sends))
        for k in (OWN, PAR):
            for dz in (1, 0, 2):
                c = far(dz, k)
                sends = []
                if dz == 1:
                    sends += [
                        (c, far(1, 1 - k), "partner", "R"),
                        (c, far(0, k), "zp", None if q in z_far else "S"),
                        (c, far(2, k), "zm", None if q in z_far else "S"),
                    ]
                if k == PAR:
                    sends.append((c, slot(2, dz, CRS), "sxd", None))
                sends.append((c, slot(2, dz, k), "sib", None))
                tasks.append(Task("relay", q, [c], sends=sends))
    tasks.append(Task("part", None, cost=3.2))
    for dz in (0, 2, 1):
        for k in (CRS, PAR, OWN):
            send = (out_slot(2, dz, k), ("RF", dz * 2 + k), "sib", None)
            if k == CRS:
                send = (out_slot(2, dz, k), ("XF", dz), "sxp", None)
            tasks.append(Task("sel", None, cost=0.03, args=(2, dz, k), sends=[send]))
    for k in (CRS, PAR, OWN):
        for dz in (0, 2, 1):
            tasks.append(Task("sel", None, cost=0.03, args=(1, dz, k), sends=[
                (out_slot(1, dz, k), ("RN", dz * 3 + k), "sib", None)]))
    for q, size in enumerate(p_sizes):
        unit = 0.14 * size / 16
        for dz in (0, 2):
            send = (("AX", dz), ("ZX", dz // 2), "zm" if dz == 0 else "zp", None)
            if q in x_near:
                send = (("AX", dz), ("XN", dz), "xp", None)
            tasks.append(Task("add", q, [("RN", dz * 3 + CRS)], cost=unit, args=(("AX", dz), dz * 3 + CRS),
                              sends=[send]))
        waits = [("RN", 3 + CRS)] + ([] if q in x_near else [("ZX", 0), ("ZX", 1)])
        tasks.append(Task("add", q, waits, cost=unit * 1.5,
                          args=(("AX", 1), 3 + CRS), sends=[(("AX", 1), ("XN", 1), "xp", None)]))
        for dz in (0, 2, 1):
            for k in (PAR, OWN):
                here = ("AF", dz * 2 + k)
                waits = [("RF", dz * 2 + k)] + ([("XF", dz)] if k == PAR else [])
                if k == PAR:
                    tasks.append(Task("add", q, waits_s=waits, role="S", cost=unit, args=(here, None), sends=[
                        (here, ("IF", dz * 2 + 1 - k), "partner", "S")]))
                else:
                    tasks.append(Task("relay", q, waits_s=waits, role="S", sends=[
                        (waits[0], ("IF", dz * 2 + 1 - k), "partner", "S")]))
                tasks.append(Task("add", q, waits_r=waits + [("IF", dz * 2 + k)], role="R", cost=unit * 1.2,
                                  args=(here, None), sends=[(here, ("EN", dz * 2 + 1 - k), "outer", "R")]))
        for dz in (0, 2):
            for k in (PAR, OWN):
                waits = [("RN", dz * 3 + k)] + ([("XN", dz)] if k == PAR and q in x_near else [])
                tasks.append(Task("add", q, waits, [("EN", dz * 2 + k)], cost=unit * 1.2,
                                  args=(("AZ", dz + k), dz * 3 + k), sends=[
                    (("AZ", dz + k), ("ZN", dz + k), "zm" if dz == 0 else "zp", None)]))
        tasks.append(Task("add", q, [("RN", 3 + PAR), ("XN", 1), ("ZN", PAR), ("ZN", 2 + PAR)],
                          [("EN", 2 + PAR)], cost=unit * 1.6, args=(("AI", 0), 3 + PAR), sends=[
            (("AI", 0), ("IN", 0), "partner", None)]))
        tasks.append(Task("add", q, [("RN", 3 + OWN), ("ZN", OWN), ("ZN", 2 + OWN), ("IN", 0)],
                          [("EN", 2 + OWN)], cost=unit * 1.6, args=(None, 3 + OWN)))
    for q, size in enumerate(d_sizes):
        tasks.append(Task("forward", q, [("H", i) for i in range(27) if i != 3], cost=0.1 + 2.7 * size / 16))
    return tasks


TOGETHER, SEND_GROUPS = 18, 3

BUFFERS = {
    "H": (28, True), "F": (6, True),
    "O": (18, False), "AX": (3, False), "AF": (6, False), "AZ": (4, False), "AI": (1, False),
    "RN": (9, False), "RF": (6, False), "XN": (3, False), "XF": (3, False), "ZX": (2, False),
    "IF": (6, False), "EN": (6, False), "ZN": (4, False), "IN": (1, False),
}


def group_of(name, index):
    if name == "H":
        return ("near", index) if index < 9 else ("sibling",)
    if name == "F":
        return (name, index)
    if name in ("RF", "XF", "IF"):
        return ("far", index * 2 + PAR if name == "XF" else index)
    if name == "ZX":
        return ("cross", 1)
    if name == "XN":
        return ("centre", PAR) if index == 1 else ("outside", index, PAR)
    if name == "IN":
        return ("centre", OWN)
    if name == "ZN":
        return ("centre", index % 2)
    dz, k = divmod(index, 3 if name == "RN" else 2)
    if k == CRS:
        return ("cross", dz)
    return ("centre", k) if dz == 1 else ("outside", dz, k)


def arrivals_of():
    numbers = {}
    for name in ("H", "F", "RN", "RF"):
        for index in range(BUFFERS[name][0]):
            for q in range(len(chunks_of(name))):
                if name != "H" or index not in (3, 27):
                    numbers.setdefault((group_of(name, index), q), len(numbers))
    return numbers


def chunks_of(name):
    sizes = D_SIZES if BUFFERS[name][1] else P_SIZES
    return [(sum(sizes[:i]), size) for i, size in enumerate(sizes)]


def places(name, rows, columns):
    unit = (rows if BUFFERS[name][1] else columns) // 16
    return [(first * unit, size * unit) for first, size in chunks_of(name)]


def kernel(off_hbm, cnt_hbm, dens_ref, tile_hbm, out_ref, *scratch):
    names = list(BUFFERS)
    halo = scratch[:len(D_SIZES)]
    scratch = scratch[len(D_SIZES):]
    buf = dict(zip(names[1:], scratch[:len(names) - 1]))
    tiles = scratch[len(names) - 1:len(names) - 1 + len(D_SIZES)]
    (square, part, flip, picked, total, back, off_ref, cnt_ref, chosen,
     local_sem, tile_sem, send_sem, recv_sem) = scratch[len(names) - 1 + len(D_SIZES):]
    gx, gy, gz = lax.axis_index("gx"), lax.axis_index("gy"), lax.axis_index("gz")
    nx, ny, nz = lax.axis_size("gx"), lax.axis_size("gy"), lax.axis_size("gz")
    b, c = lax.rem(gx, 2), lax.rem(gy, 2)
    xd = lax.rem(gx + 2 - 4 * b + nx, nx)
    xp = lax.rem(gx - 2 + 4 * b + nx, nx)
    sib = gy + 1 - 2 * c
    outer_x = lax.rem(gx + 1 - 2 * b + nx, nx)
    where_to = {
        "partner": (outer_x, gy, gz),
        "outer": (outer_x, lax.rem(gy - 2 + 4 * b + ny, ny), gz),
        "sib": (gx, sib, gz),
        "xd": (xd, gy, gz), "xp": (xp, gy, gz),
        "sxd": (xd, sib, gz), "sxp": (xp, sib, gz),
        "zp": (gx, gy, lax.rem(gz + 1, nz)),
        "zm": (gx, gy, lax.rem(gz + nz - 1, nz)),
    }
    rows, columns = total.shape
    slots = off_ref.shape[-1]
    d_places = places("H", rows, columns)

    barrier = pltpu.get_barrier_semaphore()
    for target in where_to.values():
        pl.semaphore_signal(barrier, inc=1, device_id=target, device_id_type=MESH)
    density_copies = []
    for q, (first, size) in enumerate(d_places):
        copy = pltpu.make_async_copy(
            dens_ref.at[0, 0, 0, pl.ds(first, size)], halo[q].at[3], local_sem.at[slots + q])
        copy.start()
        density_copies.append(copy)
    index_copies = [
        pltpu.make_async_copy(off_hbm, off_ref, local_sem.at[slots + len(d_places)]),
        pltpu.make_async_copy(cnt_hbm, cnt_ref, local_sem.at[slots + len(d_places) + 1]),
    ]
    for copy in index_copies:
        copy.start()

    def tile_copy(s, q):
        first, size = d_places[q]
        return pltpu.make_async_copy(
            tile_hbm.at[0, 0, 0, s, :, pl.ds(first, size)], tiles[q].at[:, pl.ds(s * size, size)],
            tile_sem.at[q])

    for s in range(slots):
        pltpu.make_async_copy(tile_hbm.at[0, 0, 0, s], square.at[s], local_sem.at[s]).start()

    def piece(name, index, q):
        if name == "H":
            return halo[q].at[index]
        first, size = places(name, rows, columns)[q]
        return buf[name].at[index, pl.ds(first, size)]

    numbers = arrivals_of()

    def arrival(name, index, q):
        return recv_sem.at[numbers[group_of(name, index), q]]

    def wait_blocks(name, n, q, semaphore):
        if BUFFERS[name][1]:
            ref = halo[q].at[pl.ds(0, n)]
        else:
            first, size = places(name, rows, columns)[q]
            ref = buf["O"].at[pl.ds(0, n), pl.ds(first, size)]
        pltpu.make_async_copy(ref, ref, semaphore).wait()

    def add(target, q, terms, own):
        first, size = places("AF", rows, columns)[q]
        strip = 32

        @pl.loop(0, size // strip)
        def _(i):
            span = pl.ds(pl.multiple_of(first + i * strip, strip), strip)
            value = None
            if own is not None:
                value = part[chosen[own], span].astype(jnp.float32)
            for name, index in terms:
                term = buf[name][index, span].astype(jnp.float32)
                value = term if value is None else value + term
            if target is None:
                back[span] = value
            else:
                buf[target[0]][target[1], span] = value.astype(jnp.bfloat16)

    def find_tiles():
        live = cnt_ref[0, 0, 0]
        home = []
        for s in range(slots):
            code = off_ref[0, 0, 0, s]
            dx, dy, dz = lax.div(code, 9), lax.rem(lax.div(code, 3), 3), lax.rem(code, 3)
            k = jnp.where(dx == 1, OWN, jnp.where(dx == 2 - 2 * b, PAR, CRS))
            group = jnp.where(dy == 1, 0, jnp.where(dy == 2 - 2 * c, 1, 2))
            home.append(jnp.where(s < live, group * 9 + dz * 3 + k, 27))
            chosen[27 + s] = home[s]

        @pl.loop(0, 27)
        def _(h):
            index = jnp.int32(slots)
            for s in range(slots):
                index = jnp.where(home[s] == h, s, index)
            chosen[h] = index

    def partials():
        for q, (first, size) in enumerate(d_places):
            flip[:, first:first + size] = halo[q][3].T
            halo[q][27] = jnp.zeros((size, columns), jnp.bfloat16)
        part[slots] = jnp.zeros((columns, rows), jnp.bfloat16)
        total[...] = jnp.zeros_like(total)
        for copy in index_copies:
            copy.wait()
        find_tiles()

        @pl.loop(0, slots)
        def _(s):
            pltpu.make_async_copy(tile_hbm.at[0, 0, 0, s], square.at[s], local_sem.at[s]).wait()
            part[s] = jnp.dot(flip[...], square[s], preferred_element_type=jnp.float32).astype(jnp.bfloat16)

        for s in range(slots):
            for q in range(len(d_places)):
                tile_copy(s, q).start()

    def forward(q):
        size = d_places[q][1]
        pltpu.make_async_copy(tiles[q], tiles[q], tile_sem.at[q]).wait()
        for s in range(slots):
            picked[s * size:(s + 1) * size] = halo[q][chosen[27 + s]]
        total[...] += jnp.dot(tiles[q][...], picked[:slots * size], preferred_element_type=jnp.float32)

    tasks = make_tasks(D_SIZES, P_SIZES, X_FIRST, Z_FAR, X_NEAR)

    def send_number(straight, q, n):
        return (q if straight else len(D_SIZES) + q) * SEND_GROUPS + n // TOGETHER

    def run(role):
        waited = set()
        sent = {}
        for number in ORDER[role]:
            task = tasks[number]
            keys = task.waits + (task.waits_s if role == "S" else task.waits_r)
            groups = {}
            for key in keys:
                if (key, task.q) not in waited:
                    waited.add((key, task.q))
                    groups.setdefault(group_of(*key), []).append(key)
            for members in groups.values():
                wait_blocks(members[0][0], len(members), task.q, arrival(*members[0], task.q))
            if task.kind == "part":
                partials()
            elif task.kind == "forward":
                forward(task.q)
            elif task.kind == "sel":
                group, dz, k = task.args
                buf["O"][(group - 1) * 9 + dz * 3 + k] = part[chosen[group * 9 + dz * 3 + k]]
            elif task.kind == "add":
                add(task.args[0], task.q, keys, task.args[1])
            elif number < len(D_SIZES):
                density_copies[number].wait()
            for source, target, to, only in task.sends:
                if only in (None, role):
                    for q in range(len(P_SIZES)) if task.q is None else [task.q]:
                        straight = BUFFERS[target[0]][1]
                        kind = (straight, q)
                        sent[kind] = sent.get(kind, 0) + 1
                        pltpu.make_async_remote_copy(
                            src_ref=piece(source[0], source[1], q),
                            dst_ref=piece(target[0], target[1], q),
                            send_sem=send_sem.at[send_number(*kind, sent[kind] - 1)],
                            recv_sem=arrival(target[0], target[1], q),
                            device_id=where_to[to],
                            device_id_type=MESH,
                        ).start()
        out_ref[0, 0, 0] = (total[...] + back[...].T).astype(out_ref.dtype)
        for (straight, q), n in sent.items():
            for first in range(0, n, TOGETHER):
                wait_blocks("H" if straight else "O", min(TOGETHER, n - first), q,
                            send_sem.at[send_number(straight, q, first)])

    pl.semaphore_wait(barrier, len(where_to))
    pl.when(b == c)(functools.partial(run, "S"))
    pl.when(b != c)(functools.partial(run, "R"))


def local(density, integrals, offsets, counts):
    rows, columns = density.shape[3:]
    slots = integrals.shape[3]
    sends = (len(D_SIZES) + len(P_SIZES)) * SEND_GROUPS
    arrivals = len(arrivals_of())
    scratch = [pltpu.VMEM((BUFFERS["H"][0], size, columns), jnp.bfloat16) for _, size in places("H", rows, columns)]
    scratch += [
        pltpu.VMEM((n, rows, columns) if straight else (n, columns, rows), jnp.bfloat16)
        for name, (n, straight) in BUFFERS.items() if name != "H"
    ]
    scratch += [
        pltpu.VMEM((rows, slots * size), jnp.bfloat16) for _, size in places("H", rows, columns)
    ]
    scratch += [
        pltpu.VMEM((slots, rows, rows), jnp.bfloat16),
        pltpu.VMEM((slots + 1, columns, rows), jnp.bfloat16),
        pltpu.VMEM((columns, rows), jnp.bfloat16),
        pltpu.VMEM((slots * max(size for _, size in places("H", rows, columns)), columns), jnp.bfloat16),
        pltpu.VMEM((rows, columns), jnp.float32),
        pltpu.VMEM((columns, rows), jnp.float32),
        pltpu.SMEM(offsets.shape, jnp.int32),
        pltpu.SMEM(counts.shape, jnp.int32),
        pltpu.SMEM((27 + slots,), jnp.int32),
        pltpu.SemaphoreType.DMA((slots + len(D_SIZES) + 2,)),
        pltpu.SemaphoreType.DMA((len(D_SIZES),)),
        pltpu.SemaphoreType.DMA((sends,)),
        pltpu.SemaphoreType.DMA((arrivals,)),
    ]
    return pl.pallas_call(
        kernel,
        out_shape=jax.ShapeDtypeStruct(density.shape, density.dtype),
        in_specs=[
            pl.BlockSpec(memory_space=pl.ANY),
            pl.BlockSpec(memory_space=pl.ANY),
            pl.BlockSpec(memory_space=pl.ANY),
            pl.BlockSpec(memory_space=pl.ANY),
        ],
        out_specs=pl.BlockSpec(memory_space=pltpu.VMEM),
        scratch_shapes=scratch,
        compiler_params=pltpu.CompilerParams(
            collective_id=0, has_side_effects=True, vmem_limit_bytes=VMEM_LIMIT
        ),
    )(offsets, counts, density, integrals)


def solution(mesh):
    return jax.shard_map(
        local,
        mesh=mesh,
        in_specs=(
            P("gx", "gy", "gz", None, None),
            P("gx", "gy", "gz", None, None, None),
            P("gx", "gy", "gz", None),
            P("gx", "gy", "gz"),
        ),
        out_specs=P("gx", "gy", "gz", None, None),
        check_vma=False,
    )
```
